256 devices in a mesh: replica: 8 (over y_lo, x), shard: 32 (over z, y_hi, core).
Axes of the slice: x: 4, y: 4 (y_hi: 2, y_lo: 2; y = y_hi * 2 + y_lo), z: 8, core: 2. Of those that a mesh axis runs over, the one named last changes fastest.
Arguments:
- tokens: bfloat16 [32768, 4096], P(('replica', 'shard')), parts along dimension 0, may hold values from -6 to 6
- queries: bfloat16 [32768, 2048], P(('replica', 'shard')), parts along dimension 0, may hold values from -48 to 48
- values: bfloat16 [32768, 512], P(('replica', 'shard')), parts along dimension 0, may hold values from -6 to 6
- out_grad: bfloat16 [32768, 2048], P(('replica', 'shard')), parts along dimension 0, may hold values from -6 to 6
- w_key: bfloat16 [32768, 512], P(('replica', 'shard')), parts along dimension 0, may hold values from -0.09375 to 0.09375
- norm_gain: bfloat16 [32768], P(('replica', 'shard')), parts along dimension 0, may hold values from 0.5 to 1.5
- key_momentum: float32 [32768, 512], P(('replica', 'shard')), parts along dimension 0, may hold values from -6 to 6
- gain_momentum: float32 [32768], P(('replica', 'shard')), parts along dimension 0, may hold values from -6 to 6
Outputs:
- attended: bfloat16 [32768, 2048], P(('replica', 'shard')), parts along dimension 0
- new_key_weight: bfloat16 [32768, 512], P(('replica', 'shard')), parts along dimension 0
- new_key_momentum: float32 [32768, 512], P(('replica', 'shard')), parts along dimension 0
- new_gain: bfloat16 [32768], P(('replica', 'shard')), parts along dimension 0
- new_gain_momentum: float32 [32768], P(('replica', 'shard')), parts along dimension 0
The draws below stay inside these ranges and needn't reach their ends.
There are 8 independent parts, one for each index of `replica`. The reference program is written for one: setup_inputs(seed, part) draws one part's arguments, and reference() takes and returns one part's arrays. A program takes and returns all parts, laid end to end along the dimension named above; each array names one. Nothing has to cross between parts.
All inputs are finite; a program needn't handle non-finite values.
Results may differ from the reference program's by a relative error of at most 0.02.
Values may be sent and summed in bfloat16 or wider, within the bound.
A program may use at most 128 MiB of HBM per device.

```python
import math
import jax
import jax.numpy as jnp
from jax import lax

D = 4096
HD = 128
HEADS = 16
KV_HEADS = 4
TOK_DEV = 128
TOKENS = 4096
N_SHARD = 32


def draw_queries(key, part):
    first_key = jax.random.fold_in(jax.random.fold_in(key, 17), 0)
    unit_draw = jax.random.truncated_normal(first_key, -6.0, 6.0, (TOKENS, HEADS * HD), jnp.float32)
    return unit_draw.astype(jnp.bfloat16)


def block_scale(stream_key, extent, cuts, least, largest):
    loudness, own = 1.0, jax.random.fold_in(stream_key, 6)
    for position, parts in cuts:
        heights = jnp.exp(jax.random.uniform(jax.random.fold_in(own, position), (parts,), jnp.float32, least / len(cuts), largest / len(cuts)))
        loudness = loudness * jnp.repeat(heights, extent[position] // parts).reshape([-1 if axis == position else 1 for axis in range(len(extent))])
    return loudness


def bell_draw(own_key, shape, scale, limit, cuts=(), held_as=jnp.bfloat16):
    array = scale * jax.random.normal(own_key, shape, jnp.float32)
    if cuts:
        array = array * block_scale(own_key, shape, cuts, -0.22, 0.18)
    return jnp.clip(array, -limit, limit).astype(held_as)


def setup_inputs(seed: int = 0, part: int = 0) -> dict:
    splits = jax.random.split(jax.random.key(seed), 9)
    part_keys = jax.random.split(jax.random.fold_in(splits[8], part), 9)
    return {
        "tokens": bell_draw(part_keys[0], (TOKENS, D), 1.0, 6.0, ((0, 32),)),
        "queries": draw_queries(jax.random.fold_in(jax.random.fold_in(splits[8], part), 71), part),
        "values": bell_draw(part_keys[2], (TOKENS, KV_HEADS * HD), 1.0, 6.0, ((0, 32),)),
        "out_grad": bell_draw(part_keys[3], (TOKENS, HEADS * HD), 1.0, 6.0, ((0, 32),)),
        "w_key": bell_draw(part_keys[4], (D, KV_HEADS * HD), D ** -0.5, 0.09375, ((0, 32),)),
        "norm_gain": jnp.clip(1.0 + 0.1 * jax.random.normal(part_keys[5], (D,), jnp.float32), 0.5, 1.5).astype(jnp.bfloat16),
        "key_momentum": bell_draw(part_keys[6], (D, KV_HEADS * HD), 1.0, 6.0, ((0, 32),), jnp.float32),
        "gain_momentum": bell_draw(part_keys[7], (D,), 1.0, 6.0, ((0, 32),), jnp.float32),
    }


epsilon = 1e-05
rope_base = 500000.0
inertia = 0.9
step_size = 0.01

def rounded(array_in):
    return lax.optimization_barrier(array_in.astype(jnp.bfloat16)).astype(jnp.float32)

def rotation_tables(positions, head_width):
    half_width = head_width // 2
    exponent = jnp.arange(half_width, dtype=jnp.float32) * (2.0 / head_width)
    frequency = jnp.exp(-math.log(rope_base) * exponent)
    angles = positions.astype(jnp.float32)[:, None] * frequency[None, :]
    return (jnp.cos(angles)[:, None, :], jnp.sin(angles)[:, None, :])

def rotate_keys(raw_rows, cosine, sine_table):
    first_half, second_half = jnp.split(raw_rows, 2, axis=-1)
    return jnp.concatenate([first_half * cosine - second_half * sine_table, second_half * cosine + first_half * sine_table], axis=-1)

def rotate_back(grad_rows, cosine, sine_table):
    first_half, second_half = jnp.split(grad_rows, 2, axis=-1)
    return jnp.concatenate([first_half * cosine + second_half * sine_table, second_half * cosine - first_half * sine_table], axis=-1)

def reference(tokens, queries, values, out_grad, w_key, norm_gain, key_momentum, gain_momentum):
    group_size = HEADS // KV_HEADS
    score_scale = HD ** (-0.5)
    inputs_float = tokens.astype(jnp.float32)
    inverse_rms = lax.rsqrt(lax.optimization_barrier(jnp.mean(inputs_float * inputs_float, axis=1, keepdims=True)) + epsilon)
    normalized = inputs_float * inverse_rms
    normed = (normalized * norm_gain.astype(jnp.float32)[None, :]).astype(jnp.bfloat16)
    raw_keys = jnp.dot(normed, w_key, preferred_element_type=jnp.float32)
    positions = jnp.arange(TOKENS, dtype=jnp.int32)
    cosine, sine_table = rotation_tables(positions, HD)
    key_rows = rotate_keys(raw_keys.reshape(TOKENS, KV_HEADS, HD), cosine, sine_table).astype(jnp.bfloat16)
    key_float = key_rows.astype(jnp.float32)
    value_float = values.reshape(TOKENS, KV_HEADS, HD).astype(jnp.float32)
    query_blocks = queries.reshape(N_SHARD, TOK_DEV, KV_HEADS, group_size, HD)
    grad_blocks = out_grad.reshape(N_SHARD, TOK_DEV, KV_HEADS, group_size, HD)

    def one_block(key_sum, inputs):
        block_number, query_block, grad_block = inputs
        query_float = query_block.astype(jnp.float32)
        grad_float = grad_block.astype(jnp.float32)
        query_pos = block_number * TOK_DEV + jnp.arange(TOK_DEV, dtype=jnp.int32)
        scores = jnp.einsum('tghd,sgd->ghts', query_float, key_float) * score_scale
        allowed = positions[None, :] <= query_pos[:, None]
        scores = jnp.where(allowed[None, None], scores, -jnp.inf)
        row_max = lax.optimization_barrier(jnp.max(scores, axis=-1))
        weights = jnp.exp(scores - row_max[..., None])
        denominator = lax.optimization_barrier(jnp.sum(weights, axis=-1))
        numerator = jnp.einsum('ghts,sgd->tghd', rounded(weights), value_float)
        attended_full = numerator / jnp.transpose(denominator, (2, 0, 1))[..., None]
        delta_rows = jnp.einsum('tghd,tghd->ght', grad_float, attended_full)
        prob_grad = jnp.einsum('tghd,sgd->ghts', grad_float, value_float)
        score_grad = weights / denominator[..., None] * (prob_grad - delta_rows[..., None])
        key_part = jnp.einsum('ghts,tghd->sgd', rounded(score_grad), query_float) * score_scale
        key_sum = key_sum + rounded(key_part)
        return (key_sum, attended_full.reshape(TOK_DEV, HEADS * HD).astype(jnp.bfloat16))
    start_sum = jnp.zeros((TOKENS, KV_HEADS, HD), jnp.float32)
    block_numbers = jnp.arange(N_SHARD, dtype=jnp.int32)
    key_grad, attended_blocks = lax.scan(one_block, start_sum, (block_numbers, query_blocks, grad_blocks))
    attended = attended_blocks.reshape(TOKENS, HEADS * HD)
    raw_grads = rotate_back(key_grad, cosine, sine_table).reshape(TOKENS, KV_HEADS * HD).astype(jnp.bfloat16)
    weight_grad = jnp.dot(normed.T, raw_grads, preferred_element_type=jnp.float32)
    normed_grad = jnp.dot(raw_grads, w_key.T, preferred_element_type=jnp.float32)
    gain_grad = lax.optimization_barrier(jnp.sum(normed_grad * normalized, axis=0))
    new_key_momentum = inertia * key_momentum + weight_grad
    new_key_weight = (w_key.astype(jnp.float32) - step_size * new_key_momentum).astype(jnp.bfloat16)
    new_gain_momentum = inertia * gain_momentum + gain_grad
    new_gain = (norm_gain.astype(jnp.float32) - step_size * new_gain_momentum).astype(jnp.bfloat16)
    return (attended, new_key_weight, new_key_momentum, new_gain, new_gain_momentum)
```

```python
import math

import jax
import jax.numpy as jnp
import numpy as np
from jax import lax
from jax.experimental import pallas as pl
from jax.experimental.pallas import tpu as pltpu
from jax.sharding import PartitionSpec as P

HD = 128
NZ = 8
NG = 4
TD = 128
CT = NG * TD
QT = 256
BOTH = ("replica", "shard")

epsilon = 1e-05
rope_base = 500000.0
inertia = 0.9
step_size = 0.01
score_scale = HD ** (-0.5)
key_fold = score_scale * math.log2(math.e)

F32 = jnp.float32
BF16 = jnp.bfloat16
MESH = pl.DeviceIdType.MESH
NT = (((1,), (1,)), ((), ()))


def rope_parts():
    half = HD // 2
    freq = np.exp(-math.log(rope_base) * np.arange(half) * (2.0 / HD))
    low = np.arange(CT)[:, None] * freq[None, :]
    high = (np.arange(NZ) * CT)[:, None] * freq[None, :]
    both = lambda a, b: np.concatenate([a, b], axis=1).astype(np.float32)
    return (
        both(np.cos(low), np.cos(low)),
        both(np.sin(low), np.sin(low)),
        both(np.cos(high), np.cos(high)),
        both(np.sin(high), np.sin(high)),
    )


def remote(src, dst, send, recv, device):
    return pltpu.make_async_remote_copy(
        src_ref=src,
        dst_ref=dst,
        send_sem=send,
        recv_sem=recv,
        device_id={"shard": device},
        device_id_type=MESH,
    )


def rows(start, size):
    return pl.ds(pl.multiple_of(start, size), size)


def kernel(
    tok_ref, q_ref, v_ref, do_ref, gw_ref, ct_ref, st_ref,
    att_ref, m_out_ref,
    w_all, tok_all, q_all, do_all, v_all, k_all, k_loc, vt_all,
    acc_k, r_loc, ot, mx, den, dlt, att_loc, dk_acc, dk_send, dk_recv,
    rg_t, mt_send, mt_recv, mt_sum, mt_x,
    w_send, w_recv, x_send, x_recv, t_send, t_recv,
    vr_send, vr_recv, kr_send, kr_recv, ka_send, ka_recv,
    dk_ssem, dk_rsem, mt_ssem, mt_rsem, at_send, at_recv, mx_send, mx_recv,
):
    me = lax.axis_index("shard")
    z = me // NG
    g = lax.rem(me, NG)
    y = g // 2
    c = lax.rem(g, 2)
    zp = lax.rem(z + 1, NZ)
    zm = lax.rem(z + NZ - 1, NZ)
    up = zp * NG + g
    down = zm * NG + g
    other_y = z * NG + (1 - y) * 2 + c
    other_c = z * NG + y * 2 + (1 - c)
    peers = [lax.rem(g + i, NG) for i in range(1, NG)]

    barrier = pltpu.get_barrier_semaphore()
    for i in range(1, NZ):
        pl.semaphore_signal(
            barrier, inc=1, device_id={"shard": lax.rem(z + i, NZ) * NG + g}, device_id_type=MESH
        )
    for p in peers:
        pl.semaphore_signal(barrier, inc=1, device_id={"shard": z * NG + p}, device_id_type=MESH)
    pl.semaphore_wait(barrier, NZ - 1 + NG - 1)

    def block(zz, yy, cc):
        return lax.rem(zz + 2 * NZ, NZ) * NG + yy * 2 + cc

    def w_copy(b, slot, device, src=None):
        here = w_all.at[rows(b * TD, TD), :]
        return remote(here if src is None else src, here, w_send.at[slot], w_recv.at[b], device)

    own = block(z, y, c)
    sends = []

    def go(copy):
        copy.start()
        sends.append(copy)

    go(w_copy(own, 0, up, gw_ref))
    go(w_copy(own, 1, down, gw_ref))
    go(w_copy(own, 2, other_y, gw_ref))
    go(w_copy(own, 3, other_c, gw_ref))
    w_all[rows(own * TD, TD), :] = gw_ref[...]

    mine = rows(g * TD, TD)
    for i, p in enumerate(peers):
        go(
            remote(
                v_ref.at[:, rows(p * HD, HD)],
                v_all.at[rows(z * CT + g * TD, TD), :],
                x_send.at[0, i], x_recv.at[0, g], z * NG + p,
            )
        )
    for k, (src, dst) in enumerate(((q_ref, q_all), (do_ref, do_all))):
        for i, p in enumerate(peers):
            go(
                remote(
                    src.at[:, rows(p * NG * HD, NG * HD)],
                    dst.at[mine, :],
                    x_send.at[1 + k, i], x_recv.at[1 + k, g], z * NG + p,
                )
            )

    def t_copy(p, slot, device, src=None):
        here = tok_all.at[rows(p * TD, TD), :]
        return remote(here if src is None else src, here, t_send.at[slot], t_recv.at[p], device)

    go(t_copy(g, 0, other_c, tok_ref))
    go(t_copy(g, 1, other_y, tok_ref))

    v_all[rows(z * CT + g * TD, TD), :] = v_ref[:, rows(g * HD, HD)]
    q_all[mine, :] = q_ref[:, rows(g * NG * HD, NG * HD)]
    do_all[mine, :] = do_ref[:, rows(g * NG * HD, NG * HD)]
    tok_all[mine, :] = tok_ref[...]

    def inverse_rms(slot):
        def add(i, s):
            t = tok_all[rows(slot * TD, TD), rows(i * 512, 512)].astype(F32)
            return s + jnp.sum(t * t, axis=1, keepdims=True)

        s = lax.fori_loop(0, tok_ref.shape[1] // 512, add, jnp.zeros((TD, 1), F32))
        return lax.rsqrt(s * (1.0 / tok_ref.shape[1]) + epsilon)

    def project(zz, yy):
        cols = rows(block(zz, yy, 0) * TD, 2 * TD)
        acc_k[...] += jnp.dot(tok_ref[:, cols], w_all[cols, :], preferred_element_type=F32)

    def w_arrived(zz, yy, cc):
        w_copy(block(zz, yy, cc), 0, up).wait_recv()

    def pass_on(zz, yy, slot):
        go_c = w_copy(block(zz, yy, c), slot, other_c)
        go_c.start()
        sends.append(go_c)

    acc_k[...] = jnp.zeros_like(acc_k)
    slot = 4
    w_arrived(z, 1 - y, c)
    go(w_copy(block(z, 1 - y, c), slot, up))
    go(w_copy(block(z, 1 - y, c), slot + 1, down))
    pass_on(z, 1 - y, slot + 2)
    slot += 3
    r_loc[...] = jnp.broadcast_to(inverse_rms(g), r_loc.shape)
    for yy in range(2):
        w_arrived(z, yy, 1 - c)
        project(z, yy)

    def ring(buf, send, recv, h):
        far_p, far_m = lax.rem(z + NZ - h, NZ), lax.rem(z + h, NZ)
        at_p, at_m = rows(far_p * CT, CT), rows(far_m * CT, CT)
        full_p = remote(buf.at[at_p, :], buf.at[at_p, :], send.at[0, h], recv.at[far_p], up)
        full_m = remote(buf.at[at_m, :], buf.at[at_m, :], send.at[1, h], recv.at[far_m], down)

        @pl.when(h > 0)
        def _():
            full_p.wait_recv()
            full_m.wait_recv()

        @pl.when(h < 3)
        def _():
            full_p.start()
            full_m.start()

        @pl.when(h == 3)
        def _():
            half_p, half_m = halves(buf, send, recv)
            half_p.start()
            half_m.start()

    def halves(buf, send, recv):
        far_p, far_m = lax.rem(z + NZ - 3, NZ), lax.rem(z + 3, NZ)
        half = CT // 2
        at_p, at_m = rows(far_p * CT, half), rows(far_m * CT + half, half)
        return (
            remote(buf.at[at_p, :], buf.at[at_p, :], send.at[0, 3], recv.at[NZ], up),
            remote(buf.at[at_m, :], buf.at[at_m, :], send.at[1, 3], recv.at[NZ + 1], down),
        )

    def ring_close(buf, send, recv):
        for copy in halves(buf, send, recv):
            copy.wait_recv()

    def ring_sent(buf, send, recv):
        for h in range(3):
            for way in range(2):
                at = rows(z * CT, CT)
                remote(buf.at[at, :], buf.at[at, :], send.at[way, h], recv.at[0], up).wait_send()
        for copy in halves(buf, send, recv):
            copy.wait_send()

    def exchanged(k, buf, at):
        for p in peers:
            here = buf.at[at(p), :]
            remote(here, here, x_send.at[k, 0], x_recv.at[k, p], other_c).wait_recv()

    for h in range(1, 5):
        for way, (sign, to) in enumerate(((-1, up), (1, down))):
            for yy in range(2):
                if h == 4 and yy != way:
                    continue
                zz = z + sign * h
                w_arrived(zz, yy, c)
                if h < 3 or (h == 3 and yy == way):
                    go(w_copy(block(zz, yy, c), slot, to))
                    slot += 1
                pass_on(zz, yy, slot)
                slot += 1
        if h == 1:
            exchanged(0, v_all, lambda p: rows(z * CT + p * TD, TD))
        ring(v_all, vr_send, vr_recv, jnp.int32(h - 1))
        for way, sign in enumerate((-1, 1)):
            for yy in range(2):
                if h == 4 and yy != way:
                    continue
                w_arrived(z + sign * h, yy, 1 - c)
                project(z + sign * h, yy)

    for p in range(NG):
        x = acc_k[:, p * HD : (p + 1) * HD] * r_loc[:, :1]
        x = x * ct_ref[mine, :] + pltpu.roll(x, HD // 2, 1) * st_ref[mine, :]
        k_loc[p] = (x * key_fold).astype(BF16)
    at_me = rows(z * CT + g * TD, TD)
    for i, p in enumerate(peers):
        go(remote(k_loc.at[p], k_all.at[at_me, :], ka_send.at[i], ka_recv.at[g], z * NG + p))
    k_all[at_me, :] = k_loc[g]
    exchanged(1, q_all, lambda p: rows(p * TD, TD))
    exchanged(2, do_all, lambda p: rows(p * TD, TD))
    for p in peers:
        here = k_all.at[rows(z * CT + p * TD, TD), :]
        remote(here, here, ka_send.at[0], ka_recv.at[p], other_c).wait_recv()

    def tiles(body):
        def step(i, carry):
            h = i // (CT // QT)
            t = lax.rem(i, CT // QT)
            body(h, t)
            return carry

        lax.fori_loop(0, NG * (CT // QT), step, 0)

    def scores(j, h, t, masked):
        k = k_all[rows(j * CT, CT), :]
        q = q_all[rows(t * QT, QT), rows(h * HD, HD)]
        s = lax.dot_general(k, q, NT, preferred_element_type=F32)
        if masked:
            key_at = lax.broadcasted_iota(jnp.int32, s.shape, 0)
            query_at = lax.broadcasted_iota(jnp.int32, s.shape, 1) + t * QT
            s = jnp.where(key_at <= query_at, s, -1e30)
        return s

    def forward(j, first):
        v_t = v_all[rows(j * CT, CT), :].astype(F32).T.astype(BF16)
        vt_all[...] = v_t

        def body(h, t):
            s = scores(j, h, t, first)
            top = jnp.max(s, axis=0, keepdims=True)
            cols = rows(t * QT, QT)
            if first:
                e = jnp.exp2(s - top)
                total = jnp.sum(e, axis=0, keepdims=True)
                out = jnp.dot(vt_all[...], e.astype(BF16), preferred_element_type=F32)
            else:
                before = mx[h, :, cols]
                top = jnp.maximum(before, top)
                fade = jnp.exp2(before - top)
                e = jnp.exp2(s - top)
                total = den[h, :, cols] * fade + jnp.sum(e, axis=0, keepdims=True)
                out = jnp.dot(vt_all[...], e.astype(BF16), preferred_element_type=F32)
                out = ot[h, :, cols] * fade + out
            mx[h, :, cols] = top
            den[h, :, cols] = total
            ot[h, :, cols] = out

        tiles(body)

    def forward_step(d, carry):
        @pl.when(d < 4)
        def _():
            ring(k_all, kr_send, kr_recv, d)

        @pl.when(d == 4)
        def _():
            ring_close(k_all, kr_send, kr_recv)

        @pl.when(d == 0)
        def _():
            ring_close(v_all, vr_send, vr_recv)
            forward(z, True)

        @pl.when(jnp.logical_and(d > 0, d <= z))
        def _():
            forward(z - d, False)

        return carry

    lax.fori_loop(0, NZ, forward_step, 0)

    for h in range(NG):
        for t in range(CT // QT):
            cols = slice(t * QT, (t + 1) * QT)
            heads = slice(h * HD, (h + 1) * HD)
            total = den[h, :, cols]
            out = ot[h, :, cols] / total
            d_out = do_all[cols, heads].astype(F32).T
            dlt[h, :, cols] = jnp.sum(out * d_out, axis=0, keepdims=True)
            mx[h, :, cols] = mx[h, :, cols] + jnp.log2(total)
            att_loc[cols, heads] = out.T.astype(BF16)
    for i, p in enumerate(peers):
        go(
            remote(
                att_loc.at[rows(p * TD, TD), :],
                att_ref.at[:, rows(g * NG * HD, NG * HD)],
                at_send.at[i], at_recv.at[g], z * NG + p,
            )
        )
    att_ref[:, rows(g * NG * HD, NG * HD)] = att_loc[mine, :]

    t_y = (1 - y) * 2 + c
    t_copy(t_y, 1, other_y).wait_recv()
    go(t_copy(t_y, 2, other_c))

    def backward(j, masked):
        dk_acc[...] = jnp.zeros_like(dk_acc)

        def body(h, t):
            cols = rows(t * QT, QT)
            heads = rows(h * HD, HD)
            p = jnp.exp2(scores(j, h, t, masked) - mx[h, :, cols])
            dp = lax.dot_general(
                v_all[rows(j * CT, CT), :], do_all[cols, heads], NT, preferred_element_type=F32
            )
            ds = (p * (dp - dlt[h, :, cols])).astype(BF16)
            dk_acc[...] += jnp.dot(ds, q_all[cols, heads], preferred_element_type=F32)

        tiles(body)

    def dk_copy(j):
        return remote(dk_send.at[j], dk_recv.at[z], dk_ssem.at[j], dk_rsem.at[z], j * NG + g)

    def backward_step(j, carry):
        backward(j, False)
        dk_send[j] = (dk_acc[...] * score_scale).astype(BF16)
        dk_copy(j).start()
        return carry

    lax.fori_loop(0, z, backward_step, 0)
    backward(z, True)
    dk_acc[...] = dk_acc[...] * score_scale

    def dk_add(i, carry):
        remote(dk_send.at[0], dk_recv.at[i], dk_ssem.at[0], dk_rsem.at[i], up).wait_recv()
        dk_acc[...] += dk_recv[i].astype(F32)
        return carry

    for p in (y * 2 + (1 - c), (1 - y) * 2 + (1 - c)):
        t_copy(p, 0, other_c).wait_recv()
    lax.fori_loop(z + 1, NZ, dk_add, 0)
    for p in range(NG):
        part = slice(p * TD, (p + 1) * TD)
        dk = dk_acc[part, :]
        raw = dk * ct_ref[part, :] - pltpu.roll(dk, HD // 2, 1) * st_ref[part, :]
        rg_t[:, part] = (raw * inverse_rms(p)).T.astype(BF16)

    def mt_copy(zz):
        return remote(mt_send.at[zz], mt_recv.at[z], mt_ssem.at[zz], mt_rsem.at[z], zz * NG + g)

    def mt_step(i, carry):
        k = lax.rem(i + NZ // 2, NZ)
        zz = lax.rem(z + k, NZ)
        part = jnp.dot(rg_t[...], tok_all[:, rows(zz * CT, CT)], preferred_element_type=F32)

        @pl.when(k == 0)
        def _():
            mt_sum[...] = part

        @pl.when(k > 0)
        def _():
            mt_send[zz] = part.astype(BF16)
            mt_copy(zz).start()

        return carry

    lax.fori_loop(0, NZ, mt_step, 0)

    def mt_add(k, carry):
        zz = lax.rem(z + k, NZ)
        remote(mt_send.at[0], mt_recv.at[zz], mt_ssem.at[0], mt_rsem.at[zz], up).wait_recv()
        mt_sum[...] += mt_recv[zz].astype(F32)
        return carry

    lax.fori_loop(1, NZ, mt_add, 0)
    for i, p in enumerate(peers):
        go(
            remote(
                mt_sum.at[:, rows(p * TD, TD)], mt_x.at[g], mx_send.at[i], mx_recv.at[g], z * NG + p
            )
        )
    m_out_ref[:, rows(g * HD, HD)] = mt_sum[:, mine].T
    for p in peers:
        remote(mt_x.at[p], mt_x.at[p], mx_send.at[0], mx_recv.at[p], other_c).wait_recv()
        m_out_ref[:, rows(p * HD, HD)] = mt_x[p].T

    for p in peers:
        there = att_ref.at[:, rows(p * NG * HD, NG * HD)]
        remote(there, there, at_send.at[0], at_recv.at[p], other_c).wait_recv()
    for copy in sends:
        copy.wait_send()
    ring_sent(v_all, vr_send, vr_recv)
    ring_sent(k_all, kr_send, kr_recv)

    def dk_sent(j, carry):
        dk_copy(j).wait_send()
        return carry

    lax.fori_loop(0, z, dk_sent, 0)

    def mt_sent(k, carry):
        mt_copy(lax.rem(z + k, NZ)).wait_send()
        return carry

    lax.fori_loop(1, NZ, mt_sent, 0)


def call(tokens, queries, values, out_grad, scaled, ct, st):
    width, key_width = tokens.shape[1], values.shape[1]
    dma = pltpu.SemaphoreType.DMA
    vmem = lambda shape, dtype: pltpu.VMEM(shape, dtype)
    tokens_all = NZ * CT
    return pl.pallas_call(
        kernel,
        out_shape=(
            jax.ShapeDtypeStruct(queries.shape, BF16),
            jax.ShapeDtypeStruct((TD, key_width), F32),
        ),
        in_specs=[pl.BlockSpec(memory_space=pltpu.VMEM)] * 7,
        out_specs=(pl.BlockSpec(memory_space=pltpu.VMEM),) * 2,
        scratch_shapes=[
            vmem((width, key_width), BF16),
            vmem((CT, width), BF16),
            vmem((CT, NG * HD), BF16),
            vmem((CT, NG * HD), BF16),
            vmem((tokens_all, HD), BF16),
            vmem((tokens_all, HD), BF16),
            vmem((NG, TD, HD), BF16),
            vmem((HD, CT), BF16),
            vmem((TD, key_width), F32),
            vmem((TD, 128), F32),
            vmem((NG, HD, CT), F32),
            vmem((NG, 1, CT), F32),
            vmem((NG, 1, CT), F32),
            vmem((NG, 1, CT), F32),
            vmem((CT, NG * HD), BF16),
            vmem((CT, HD), F32),
            vmem((NZ, CT, HD), BF16),
            vmem((NZ, CT, HD), BF16),
            vmem((HD, CT), BF16),
            vmem((NZ, HD, CT), BF16),
            vmem((NZ, HD, CT), BF16),
            vmem((HD, CT), F32),
            vmem((NG, HD, TD), F32),
            dma((32,)), dma((32,)),
            dma((3, 3)), dma((3, NG)),
            dma((3,)), dma((NG,)),
            dma((2, 4)), dma((NZ + 2,)),
            dma((2, 4)), dma((NZ + 2,)),
            dma((3,)), dma((NG,)),
            dma((NZ,)), dma((NZ,)),
            dma((NZ,)), dma((NZ,)),
            dma((3,)), dma((NG,)),
            dma((3,)), dma((NG,)),
        ],
        compiler_params=pltpu.CompilerParams(
            collective_id=0, has_side_effects=True, vmem_limit_bytes=56 << 20
        ),
    )(tokens, queries, values, out_grad, scaled, ct, st)


def shards(tokens, queries, values, out_grad, w_key, norm_gain, key_momentum, gain_momentum):
    z = lax.axis_index("shard") // NG
    cl, sl, ch, sh = (jnp.asarray(a) for a in rope_parts())
    ch, sh = (lax.dynamic_slice_in_dim(a, z, 1, 0) for a in (ch, sh))
    sign = jnp.where(jnp.arange(HD) < HD // 2, -1.0, 1.0).astype(F32)[None, :]
    ct = cl * ch - sl * sh
    st = (sl * ch + cl * sh) * sign
    w = w_key.astype(F32)
    gain = norm_gain.astype(F32)
    scaled = (w * gain[:, None]).astype(BF16)
    attended, m = call(tokens, queries, values, out_grad, scaled, ct, st)
    new_key_momentum = inertia * key_momentum + gain[:, None] * m
    new_key_weight = (w - step_size * new_key_momentum).astype(BF16)
    new_gain_momentum = inertia * gain_momentum + jnp.sum(w * m, axis=1)
    new_gain = (gain - step_size * new_gain_momentum).astype(BF16)
    return (attended, new_key_weight, new_key_momentum, new_gain, new_gain_momentum)


def solution(mesh):
    both, flat = P(BOTH, None), P(BOTH)
    return jax.shard_map(
        shards,
        mesh=mesh,
        in_specs=(both, both, both, both, both, flat, both, flat),
        out_specs=(both, both, both, flat, flat),
        check_vma=False,
    )
```

```python
import math

import jax
import jax.numpy as jnp
import numpy as np
from jax import lax
from jax.experimental import pallas as pl
from jax.experimental.pallas import tpu as pltpu
from jax.sharding import PartitionSpec as P

HD = 128
NZ = 8
NG = 4
TD = 128
CT = NG * TD
QT = 256
BOTH = ("replica", "shard")

epsilon = 1e-05
rope_base = 500000.0
inertia = 0.9
step_size = 0.01
score_scale = HD ** (-0.5)
key_fold = score_scale * math.log2(math.e)

F32 = jnp.float32
BF16 = jnp.bfloat16
MESH = pl.DeviceIdType.MESH
NT = (((1,), (1,)), ((), ()))


def rope_parts():
    half = HD // 2
    freq = np.exp(-math.log(rope_base) * np.arange(half) * (2.0 / HD))
    low = np.arange(CT)[:, None] * freq[None, :]
    high = (np.arange(NZ) * CT)[:, None] * freq[None, :]
    both = lambda a, b: np.concatenate([a, b], axis=1).astype(np.float32)
    return (
        both(np.cos(low), np.cos(low)),
        both(np.sin(low), np.sin(low)),
        both(np.cos(high), np.cos(high)),
        both(np.sin(high), np.sin(high)),
    )


def remote(src, dst, send, recv, device):
    return pltpu.make_async_remote_copy(
        src_ref=src,
        dst_ref=dst,
        send_sem=send,
        recv_sem=recv,
        device_id={"shard": device},
        device_id_type=MESH,
    )


def rows(start, size):
    return pl.ds(pl.multiple_of(start, size), size)


def kernel(
    tok_ref, q_ref, v_ref, do_ref, w_ref, gain_ref, cl_ref, sl_ref, ch_ref, sh_ref,
    att_ref, m_out_ref,
    w_all, tok_all, q_all, do_all, v_all, k_all, k_loc, vt_all,
    acc_k, ct_ref, st_ref, r_all, ot, mx, den, dlt, att_loc, dk_acc, dk_send, dk_recv,
    rg_t, mt_far, mt_got, mt_send, mt_recv, mt_part, mt_sum, mt_x,
    w_send, w_recv, x_send, x_recv, t_send, t_recv, r_send, r_recv,
    vr_send, vr_recv, kr_send, kr_recv, ka_send, ka_recv,
    dk_ssem, dk_rsem, mt_ssem, mt_rsem, at_send, at_recv, mx_send, mx_recv,
):
    me = lax.axis_index("shard")
    z = me // NG
    g = lax.rem(me, NG)
    y = g // 2
    c = lax.rem(g, 2)
    zp = lax.rem(z + 1, NZ)
    zm = lax.rem(z + NZ - 1, NZ)
    up = zp * NG + g
    down = zm * NG + g
    other_y = z * NG + (1 - y) * 2 + c
    other_c = z * NG + y * 2 + (1 - c)
    peers = [lax.rem(g + i, NG) for i in range(1, NG)]

    own_w = rows(me * TD, TD)
    gain = jnp.broadcast_to(gain_ref[...], (TD, TD)).T
    for h in range(NG):
        cols = slice(h * HD, (h + 1) * HD)
        w_all[own_w, cols] = (w_ref[:, cols].astype(F32) * gain).astype(BF16)

    barrier = pltpu.get_barrier_semaphore()
    for i in range(1, NZ):
        pl.semaphore_signal(
            barrier, inc=1, device_id={"shard": lax.rem(z + i, NZ) * NG + g}, device_id_type=MESH
        )
    for p in peers:
        pl.semaphore_signal(barrier, inc=1, device_id={"shard": z * NG + p}, device_id_type=MESH)
    pl.semaphore_wait(barrier, NZ - 1 + NG - 1)

    def block(zz, yy, cc):
        return lax.rem(zz + 2 * NZ, NZ) * NG + yy * 2 + cc

    def w_copy(b, slot, device):
        here = w_all.at[rows(b * TD, TD), :]
        return remote(here, here, w_send.at[slot], w_recv.at[b], device)

    sends = []

    def go(copy):
        copy.start()
        sends.append(copy)

    for i, to in enumerate((up, down, other_y, other_c)):
        go(w_copy(me, i, to))

    mine = rows(g * TD, TD)
    for i, p in enumerate(peers):
        go(
            remote(
                v_ref.at[:, rows(p * HD, HD)],
                v_all.at[rows(z * CT + g * TD, TD), :],
                x_send.at[0, i], x_recv.at[0, g], z * NG + p,
            )
        )
    for k, (src, dst) in enumerate(((q_ref, q_all), (do_ref, do_all))):
        for i, p in enumerate(peers):
            go(
                remote(
                    src.at[:, rows(p * NG * HD, NG * HD)],
                    dst.at[mine, :],
                    x_send.at[1 + k, i], x_recv.at[1 + k, g], z * NG + p,
                )
            )

    def t_copy(p, slot, device, src=None):
        here = tok_all.at[rows(p * TD, TD), :]
        return remote(here if src is None else src, here, t_send.at[slot], t_recv.at[p], device)

    go(t_copy(g, 0, other_c, tok_ref))
    go(t_copy(g, 1, other_y, tok_ref))

    v_all[rows(z * CT + g * TD, TD), :] = v_ref[:, rows(g * HD, HD)]
    q_all[mine, :] = q_ref[:, rows(g * NG * HD, NG * HD)]
    do_all[mine, :] = do_ref[:, rows(g * NG * HD, NG * HD)]
    tok_all[mine, :] = tok_ref[...]

    def add_squares(i, total):
        t = tok_ref[:, rows(i * 512, 512)].astype(F32)
        return total + jnp.sum(t * t, axis=1, keepdims=True)

    width = tok_ref.shape[1]
    squares = lax.fori_loop(0, width // 512, add_squares, jnp.zeros((TD, 1), F32))
    r_all[mine, :] = jnp.broadcast_to(lax.rsqrt(squares * (1.0 / width) + epsilon), (TD, HD))

    def r_copy(p, i, device):
        here = r_all.at[rows(p * TD, TD), :]
        return remote(here, here, r_send.at[i], r_recv.at[p], device)

    for i, p in enumerate(peers):
        go(r_copy(g, i, z * NG + p))

    def project(zz, yy):
        cols = rows(block(zz, yy, 0) * TD, 2 * TD)
        acc_k[...] += jnp.dot(tok_ref[:, cols], w_all[cols, :], preferred_element_type=F32)

    def w_arrived(zz, yy, cc):
        w_copy(block(zz, yy, cc), 0, up).wait_recv()

    slot = 4

    def forward_w(h, yy, way):
        nonlocal slot
        zz = z + (-h if way == 0 else h)
        w_arrived(zz, yy, c)
        if h < 3 or (h == 3 and (way == 0) == (yy is own_y)):
            go(w_copy(block(zz, yy, c), slot, up if way == 0 else down))
            slot += 1
        go(w_copy(block(zz, yy, c), slot, other_c))
        slot += 1

    own_y, far_y = y, 1 - y
    acc_k[...] = jnp.zeros_like(acc_k)

    def ring(buf, send, recv, h):
        far_p, far_m = lax.rem(z + NZ - h, NZ), lax.rem(z + h, NZ)
        at_p, at_m = rows(far_p * CT, CT), rows(far_m * CT, CT)
        full_p = remote(buf.at[at_p, :], buf.at[at_p, :], send.at[0, h], recv.at[far_p], up)
        full_m = remote(buf.at[at_m, :], buf.at[at_m, :], send.at[1, h], recv.at[far_m], down)

        @pl.when(h > 0)
        def _():
            full_p.wait_recv()
            full_m.wait_recv()

        @pl.when(h < 3)
        def _():
            full_p.start()
            full_m.start()

        @pl.when(h == 3)
        def _():
            half_p, half_m = halves(buf, send, recv)
            half_p.start()
            half_m.start()

    def halves(buf, send, recv):
        far_p, far_m = lax.rem(z + NZ - 3, NZ), lax.rem(z + 3, NZ)
        half = CT // 2
        at_p, at_m = rows(far_p * CT, half), rows(far_m * CT + half, half)
        return (
            remote(buf.at[at_p, :], buf.at[at_p, :], send.at[0, 3], recv.at[NZ], up),
            remote(buf.at[at_m, :], buf.at[at_m, :], send.at[1, 3], recv.at[NZ + 1], down),
        )

    def ring_close(buf, send, recv):
        for copy in halves(buf, send, recv):
            copy.wait_recv()

    def ring_sent(buf, send, recv):
        for h in range(3):
            for way in range(2):
                at = rows(z * CT, CT)
                remote(buf.at[at, :], buf.at[at, :], send.at[way, h], recv.at[0], up).wait_send()
        for copy in halves(buf, send, recv):
            copy.wait_send()

    def exchanged(k, buf, at):
        for p in peers:
            here = buf.at[at(p), :]
            remote(here, here, x_send.at[k, 0], x_recv.at[k, p], other_c).wait_recv()

    def project_at(zz, ys):
        for yy in ys:
            w_arrived(zz, yy, 1 - c)
            project(zz, yy)

    for way in range(2):
        forward_w(1, own_y, way)
    w_arrived(z, far_y, c)
    for to in (up, down, other_c):
        go(w_copy(block(z, far_y, c), slot, to))
        slot += 1
    high = (ch_ref[pl.ds(z, 1), :], sh_ref[pl.ds(z, 1), :])
    sign = jnp.where(lax.broadcasted_iota(jnp.int32, (1, HD), 1) < HD // 2, -1.0, 1.0)
    ct_ref[...] = cl_ref[...] * high[0] - sl_ref[...] * high[1]
    st_ref[...] = (sl_ref[...] * high[0] + cl_ref[...] * high[1]) * sign
    project_at(z, (own_y, far_y))
    for h in range(1, 4):
        for way in range(2):
            if h < 3 or way == 0:
                forward_w(h + 1, own_y, way)
        for way in range(2):
            forward_w(h, far_y, way)
        if h == 3:
            exchanged(0, v_all, lambda p: rows(z * CT + p * TD, TD))
            ring(v_all, vr_send, vr_recv, jnp.int32(0))
        for sign in (-1, 1):
            project_at(z + sign * h, (own_y, far_y))
    forward_w(4, far_y, 1)
    project_at(z - 4, (own_y,))
    project_at(z + 4, (far_y,))
    ring(v_all, vr_send, vr_recv, jnp.int32(1))

    for p in range(NG):
        x = acc_k[:, p * HD : (p + 1) * HD] * r_all[mine, :]
        x = x * ct_ref[mine, :] + pltpu.roll(x, HD // 2, 1) * st_ref[mine, :]
        k_loc[p] = (x * key_fold).astype(BF16)
    at_me = rows(z * CT + g * TD, TD)
    for i, p in enumerate(peers):
        go(remote(k_loc.at[p], k_all.at[at_me, :], ka_send.at[i], ka_recv.at[g], z * NG + p))
    k_all[at_me, :] = k_loc[g]
    ring(v_all, vr_send, vr_recv, jnp.int32(2))
    exchanged(1, q_all, lambda p: rows(p * TD, TD))
    exchanged(2, do_all, lambda p: rows(p * TD, TD))
    for p in peers:
        here = k_all.at[rows(z * CT + p * TD, TD), :]
        remote(here, here, ka_send.at[0], ka_recv.at[p], other_c).wait_recv()

    ring(v_all, vr_send, vr_recv, jnp.int32(3))

    def tiles(body):
        def step(i, carry):
            h = i // (CT // QT)
            t = lax.rem(i, CT // QT)
            body(h, t)
            return carry

        lax.fori_loop(0, NG * (CT // QT), step, 0)

    def scores(j, h, t, masked):
        k = k_all[rows(j * CT, CT), :]
        q = q_all[rows(t * QT, QT), rows(h * HD, HD)]
        s = lax.dot_general(k, q, NT, preferred_element_type=F32)
        if masked:
            key_at = lax.broadcasted_iota(jnp.int32, s.shape, 0)
            query_at = lax.broadcasted_iota(jnp.int32, s.shape, 1) + t * QT
            s = jnp.where(key_at <= query_at, s, -1e30)
        return s

    def forward(j, first):
        v_t = v_all[rows(j * CT, CT), :].astype(F32).T.astype(BF16)
        vt_all[...] = v_t

        def body(h, t):
            s = scores(j, h, t, first)
            top = jnp.max(s, axis=0, keepdims=True)
            cols = rows(t * QT, QT)
            if first:
                e = jnp.exp2(s - top)
                total = jnp.sum(e, axis=0, keepdims=True)
                out = jnp.dot(vt_all[...], e.astype(BF16), preferred_element_type=F32)
            else:
                before = mx[h, :, cols]
                top = jnp.maximum(before, top)
                fade = jnp.exp2(before - top)
                e = jnp.exp2(s - top)
                total = den[h, :, cols] * fade + jnp.sum(e, axis=0, keepdims=True)
                out = jnp.dot(vt_all[...], e.astype(BF16), preferred_element_type=F32)
                out = ot[h, :, cols] * fade + out
            mx[h, :, cols] = top
            den[h, :, cols] = total
            ot[h, :, cols] = out

        tiles(body)

    def forward_step(d, carry):
        @pl.when(d < 4)
        def _():
            ring(k_all, kr_send, kr_recv, d)

        @pl.when(d == 4)
        def _():
            ring_close(v_all, vr_send, vr_recv)
            ring_close(k_all, kr_send, kr_recv)

        @pl.when(d == 0)
        def _():
            forward(z, True)

        @pl.when(jnp.logical_and(d > 0, d <= z))
        def _():
            forward(z - d, False)

        return carry

    lax.fori_loop(0, NZ, forward_step, 0)

    for h in range(NG):
        for t in range(CT // QT):
            cols = slice(t * QT, (t + 1) * QT)
            heads = slice(h * HD, (h + 1) * HD)
            total = den[h, :, cols]
            out = ot[h, :, cols] / total
            d_out = do_all[cols, heads].astype(F32).T
            dlt[h, :, cols] = jnp.sum(out * d_out, axis=0, keepdims=True)
            mx[h, :, cols] = mx[h, :, cols] + jnp.log2(total)
            att_loc[cols, heads] = out.T.astype(BF16)
    for i, p in enumerate(peers):
        go(
            remote(
                att_loc.at[rows(p * TD, TD), :],
                att_ref.at[:, rows(g * NG * HD, NG * HD)],
                at_send.at[i], at_recv.at[g], z * NG + p,
            )
        )
    att_ref[:, rows(g * NG * HD, NG * HD)] = att_loc[mine, :]

    t_y = (1 - y) * 2 + c
    t_copy(t_y, 1, other_y).wait_recv()
    go(t_copy(t_y, 2, other_c))

    def backward(j, masked):
        dk_acc[...] = jnp.zeros_like(dk_acc)

        def body(h, t):
            cols = rows(t * QT, QT)
            heads = rows(h * HD, HD)
            p = jnp.exp2(scores(j, h, t, masked) - mx[h, :, cols])
            dp = lax.dot_general(
                v_all[rows(j * CT, CT), :], do_all[cols, heads], NT, preferred_element_type=F32
            )
            ds = (p * (dp - dlt[h, :, cols])).astype(BF16)
            dk_acc[...] += jnp.dot(ds, q_all[cols, heads], preferred_element_type=F32)

        tiles(body)

    def dk_copy(j):
        return remote(dk_send.at[j], dk_recv.at[z], dk_ssem.at[j], dk_rsem.at[z], j * NG + g)

    def backward_step(j, carry):
        backward(j, False)
        dk_send[j] = (dk_acc[...] * score_scale).astype(BF16)
        dk_copy(j).start()
        return carry

    lax.fori_loop(0, z, backward_step, 0)
    backward(z, True)
    dk_acc[...] = dk_acc[...] * score_scale

    def dk_add(i, carry):
        remote(dk_send.at[0], dk_recv.at[i], dk_ssem.at[0], dk_rsem.at[i], up).wait_recv()
        dk_acc[...] += dk_recv[i].astype(F32)
        return carry

    for p in (y * 2 + (1 - c), (1 - y) * 2 + (1 - c)):
        t_copy(p, 0, other_c).wait_recv()
    for p in peers:
        r_copy(p, 0, other_c).wait_recv()
    lax.fori_loop(z + 1, NZ, dk_add, 0)
    for p in range(NG):
        part = slice(p * TD, (p + 1) * TD)
        dk = dk_acc[part, :]
        raw = dk * ct_ref[part, :] - pltpu.roll(dk, HD // 2, 1) * st_ref[part, :]
        rg_t[:, part] = (raw * r_all[part, :]).T.astype(BF16)

    half_k, half_f = HD // 2, CT // 2
    ways = ((0, up), (1, down))

    def term(zz):
        return jnp.dot(rg_t[...], tok_all[:, rows(zz * CT, CT)], preferred_element_type=F32)

    def mt_copy(s, way, k, to):
        src, dst = (mt_far, mt_got) if s == 0 else (mt_send.at[s - 1], mt_recv.at[s - 1])
        return remote(
            src.at[way, k], dst.at[way, k], mt_ssem.at[s, way, k], mt_rsem.at[s, way, k], to
        )

    far = term(lax.rem(z + 4, NZ))
    for k in range(2):
        for way, to in ways:
            part = slice(k * half_k, (k + 1) * half_k)
            mt_far[way, k] = far[part, way * half_f : (way + 1) * half_f].astype(BF16)
            go(mt_copy(0, way, k, to))
    for s in range(1, 4):
        for way, to in ways:
            mt_part[way] = term(lax.rem(z + (4 - s if way == 0 else 4 + s), NZ))
        for k in range(2):
            part = slice(k * half_k, (k + 1) * half_k)
            for way, to in ways:
                mt_copy(s - 1, way, k, to).wait_recv()
                if s == 1:
                    near = slice(way * half_f, (way + 1) * half_f)
                    mt_part[way, part, near] += mt_got[way, k].astype(F32)
                else:
                    mt_part[way, part, :] += mt_recv[s - 2, way, k].astype(F32)
                mt_send[s - 1, way, k] = mt_part[way, part, :].astype(BF16)
                go(mt_copy(s, way, k, to))
    mt_sum[...] = term(z)
    for k in range(2):
        part = slice(k * half_k, (k + 1) * half_k)
        for way, to in ways:
            mt_copy(3, way, k, to).wait_recv()
            mt_sum[part, :] += mt_recv[2, way, k].astype(F32)
    for i, p in enumerate(peers):
        go(
            remote(
                mt_sum.at[:, rows(p * TD, TD)], mt_x.at[g], mx_send.at[i], mx_recv.at[g], z * NG + p
            )
        )
    m_out_ref[:, rows(g * HD, HD)] = mt_sum[:, mine].T
    for p in peers:
        remote(mt_x.at[p], mt_x.at[p], mx_send.at[0], mx_recv.at[p], other_c).wait_recv()
        m_out_ref[:, rows(p * HD, HD)] = mt_x[p].T

    for p in peers:
        there = att_ref.at[:, rows(p * NG * HD, NG * HD)]
        remote(there, there, at_send.at[0], at_recv.at[p], other_c).wait_recv()
    for copy in sends:
        copy.wait_send()
    ring_sent(v_all, vr_send, vr_recv)
    ring_sent(k_all, kr_send, kr_recv)

    def dk_sent(j, carry):
        dk_copy(j).wait_send()
        return carry

    lax.fori_loop(0, z, dk_sent, 0)


def call(tokens, queries, values, out_grad, w_key, gain):
    width, key_width = tokens.shape[1], values.shape[1]
    dma = pltpu.SemaphoreType.DMA
    vmem = lambda shape, dtype: pltpu.VMEM(shape, dtype)
    tokens_all = NZ * CT
    return pl.pallas_call(
        kernel,
        out_shape=(
            jax.ShapeDtypeStruct(queries.shape, BF16),
            jax.ShapeDtypeStruct((TD, key_width), F32),
        ),
        in_specs=[pl.BlockSpec(memory_space=pltpu.VMEM)] * 10,
        out_specs=(pl.BlockSpec(memory_space=pltpu.VMEM),) * 2,
        scratch_shapes=[
            vmem((width, key_width), BF16),
            vmem((CT, width), BF16),
            vmem((CT, NG * HD), BF16),
            vmem((CT, NG * HD), BF16),
            vmem((tokens_all, HD), BF16),
            vmem((tokens_all, HD), BF16),
            vmem((NG, TD, HD), BF16),
            vmem((HD, CT), BF16),
            vmem((TD, key_width), F32),
            vmem((CT, HD), F32),
            vmem((CT, HD), F32),
            vmem((CT, HD), F32),
            vmem((NG, HD, CT), F32),
            vmem((NG, 1, CT), F32),
            vmem((NG, 1, CT), F32),
            vmem((NG, 1, CT), F32),
            vmem((CT, NG * HD), BF16),
            vmem((CT, HD), F32),
            vmem((NZ, CT, HD), BF16),
            vmem((NZ, CT, HD), BF16),
            vmem((HD, CT), BF16),
            vmem((2, 2, HD // 2, CT // 2), BF16),
            vmem((2, 2, HD // 2, CT // 2), BF16),
            vmem((3, 2, 2, HD // 2, CT), BF16),
            vmem((3, 2, 2, HD // 2, CT), BF16),
            vmem((2, HD, CT), F32),
            vmem((HD, CT), F32),
            vmem((NG, HD, TD), F32),
            dma((32,)), dma((32,)),
            dma((3, 3)), dma((3, NG)),
            dma((3,)), dma((NG,)),
            dma((3,)), dma((NG,)),
            dma((2, 4)), dma((NZ + 2,)),
            dma((2, 4)), dma((NZ + 2,)),
            dma((3,)), dma((NG,)),
            dma((NZ,)), dma((NZ,)),
            dma((4, 2, 2)), dma((4, 2, 2)),
            dma((3,)), dma((NG,)),
            dma((3,)), dma((NG,)),
        ],
        compiler_params=pltpu.CompilerParams(
            collective_id=0, has_side_effects=True, vmem_limit_bytes=56 << 20
        ),
    )(tokens, queries, values, out_grad, w_key, gain, *map(jnp.asarray, rope_parts()))


def shards(tokens, queries, values, out_grad, w_key, norm_gain, key_momentum, gain_momentum):
    w = w_key.astype(F32)
    gain = norm_gain.astype(F32)
    attended, m = call(tokens, queries, values, out_grad, w_key, gain[None, :])
    new_key_momentum = inertia * key_momentum + gain[:, None] * m
    new_key_weight = (w - step_size * new_key_momentum).astype(BF16)
    new_gain_momentum = inertia * gain_momentum + jnp.sum(w * m, axis=1)
    new_gain = (gain - step_size * new_gain_momentum).astype(BF16)
    return (attended, new_key_weight, new_key_momentum, new_gain, new_gain_momentum)


def solution(mesh):
    both, flat = P(BOTH, None), P(BOTH)
    return jax.shard_map(
        shards,
        mesh=mesh,
        in_specs=(both, both, both, both, both, flat, both, flat),
        out_specs=(both, both, both, flat, flat),
        check_vma=False,
    )
```

```python
import math

import jax
import jax.numpy as jnp
import numpy as np
from jax import lax
from jax.experimental import pallas as pl
from jax.experimental.pallas import tpu as pltpu
from jax.sharding import PartitionSpec as P

HD = 128
NZ = 8
NG = 4
TD = 128
CT = NG * TD
QT = 256
BOTH = ("replica", "shard")

epsilon = 1e-05
rope_base = 500000.0
inertia = 0.9
step_size = 0.01
score_scale = HD ** (-0.5)
key_fold = score_scale * math.log2(math.e)

F32 = jnp.float32
BF16 = jnp.bfloat16
MESH = pl.DeviceIdType.MESH
NT = (((1,), (1,)), ((), ()))


def rope_parts():
    half = HD // 2
    freq = np.exp(-math.log(rope_base) * np.arange(half) * (2.0 / HD))
    low = np.arange(CT)[:, None] * freq[None, :]
    high = (np.arange(NZ) * CT)[:, None] * freq[None, :]
    both = lambda a, b: np.concatenate([a, b], axis=1).astype(np.float32)
    return (
        both(np.cos(low), np.cos(low)),
        both(np.sin(low), np.sin(low)),
        both(np.cos(high), np.cos(high)),
        both(np.sin(high), np.sin(high)),
    )


def remote(src, dst, send, recv, device):
    return pltpu.make_async_remote_copy(
        src_ref=src,
        dst_ref=dst,
        send_sem=send,
        recv_sem=recv,
        device_id={"shard": device},
        device_id_type=MESH,
    )


def rows(start, size):
    return pl.ds(pl.multiple_of(start, size), size)


def kernel(
    tok_ref, q_ref, v_ref, do_ref, w_ref, gain_ref, cl_ref, sl_ref, ch_ref, sh_ref,
    att_ref, m_out_ref,
    w_all, tok_all, q_all, do_all, v_all, k_all, k_loc, vt_all,
    acc_k, ct_ref, st_ref, r_all, ot, mx, den, dlt, att_loc, dk_acc, dk_send, dk_recv,
    rg_t, mt_far, mt_got, mt_send, mt_recv, mt_part, mt_sum, mt_x,
    w_send, w_recv, x_send, x_recv, t_send, t_recv, r_send, r_recv,
    vr_send, vr_recv, kr_send, kr_recv, ka_send, ka_recv,
    dk_ssem, dk_rsem, mt_ssem, mt_rsem, at_send, at_recv, mx_send, mx_recv,
):
    me = lax.axis_index("shard")
    z = me // NG
    g = lax.rem(me, NG)
    y = g // 2
    c = lax.rem(g, 2)
    zp = lax.rem(z + 1, NZ)
    zm = lax.rem(z + NZ - 1, NZ)
    up = zp * NG + g
    down = zm * NG + g
    other_y = z * NG + (1 - y) * 2 + c
    other_c = z * NG + y * 2 + (1 - c)
    peers = [lax.rem(g + i, NG) for i in range(1, NG)]

    own_w = rows(me * TD, TD)
    gain = jnp.broadcast_to(gain_ref[...], (TD, TD)).T
    for h in range(NG):
        cols = slice(h * HD, (h + 1) * HD)
        w_all[own_w, cols] = (w_ref[:, cols].astype(F32) * gain).astype(BF16)

    barrier = pltpu.get_barrier_semaphore()
    for i in range(1, NZ):
        pl.semaphore_signal(
            barrier, inc=1, device_id={"shard": lax.rem(z + i, NZ) * NG + g}, device_id_type=MESH
        )
    for p in peers:
        pl.semaphore_signal(barrier, inc=1, device_id={"shard": z * NG + p}, device_id_type=MESH)
    pl.semaphore_wait(barrier, NZ - 1 + NG - 1)

    def block(zz, yy, cc):
        return lax.rem(zz + 2 * NZ, NZ) * NG + yy * 2 + cc

    def w_copy(b, slot, device):
        here = w_all.at[rows(b * TD, TD), :]
        return remote(here, here, w_send.at[slot], w_recv.at[b], device)

    sends = []

    def go(copy):
        copy.start()
        sends.append(copy)

    for i, to in enumerate((up, down, other_y, other_c)):
        go(w_copy(me, i, to))

    mine = rows(g * TD, TD)
    for i, p in enumerate(peers):
        go(
            remote(
                v_ref.at[:, rows(p * HD, HD)],
                v_all.at[rows(z * CT + g * TD, TD), :],
                x_send.at[0, i], x_recv.at[0, g], z * NG + p,
            )
        )

    def spread(k, src, dst):
        for i, p in enumerate(peers):
            go(
                remote(
                    src.at[:, rows(p * NG * HD, NG * HD)],
                    dst.at[mine, :],
                    x_send.at[k, i], x_recv.at[k, g], z * NG + p,
                )
            )

    spread(1, q_ref, q_all)

    def t_copy(p, slot, device, src=None):
        here = tok_all.at[rows(p * TD, TD), :]
        return remote(here if src is None else src, here, t_send.at[slot], t_recv.at[p], device)

    v_all[rows(z * CT + g * TD, TD), :] = v_ref[:, rows(g * HD, HD)]
    q_all[mine, :] = q_ref[:, rows(g * NG * HD, NG * HD)]
    do_all[mine, :] = do_ref[:, rows(g * NG * HD, NG * HD)]
    tok_all[mine, :] = tok_ref[...]

    def add_squares(i, total):
        t = tok_ref[:, rows(i * 512, 512)].astype(F32)
        return total + jnp.sum(t * t, axis=1, keepdims=True)

    width = tok_ref.shape[1]
    squares = lax.fori_loop(0, width // 512, add_squares, jnp.zeros((TD, 1), F32))
    r_all[mine, :] = jnp.broadcast_to(lax.rsqrt(squares * (1.0 / width) + epsilon), (TD, HD))

    def r_copy(p, i, device):
        here = r_all.at[rows(p * TD, TD), :]
        return remote(here, here, r_send.at[i], r_recv.at[p], device)

    def project(zz, yy):
        cols = rows(block(zz, yy, 0) * TD, 2 * TD)
        acc_k[...] += jnp.dot(tok_ref[:, cols], w_all[cols, :], preferred_element_type=F32)

    def w_arrived(zz, yy, cc):
        w_copy(block(zz, yy, cc), 0, up).wait_recv()

    slot = 4

    def forward_w(h, yy, way):
        nonlocal slot
        zz = z + (-h if way == 0 else h)
        w_arrived(zz, yy, c)
        if h < 3 or (h == 3 and (way == 0) == (yy is own_y)):
            go(w_copy(block(zz, yy, c), slot, up if way == 0 else down))
            slot += 1
        go(w_copy(block(zz, yy, c), slot, other_c))
        slot += 1

    own_y, far_y = y, 1 - y
    acc_k[...] = jnp.zeros_like(acc_k)

    def ring(buf, send, recv, h):
        far_p, far_m = lax.rem(z + NZ - h, NZ), lax.rem(z + h, NZ)
        at_p, at_m = rows(far_p * CT, CT), rows(far_m * CT, CT)
        full_p = remote(buf.at[at_p, :], buf.at[at_p, :], send.at[0, h], recv.at[far_p], up)
        full_m = remote(buf.at[at_m, :], buf.at[at_m, :], send.at[1, h], recv.at[far_m], down)

        @pl.when(h > 0)
        def _():
            full_p.wait_recv()
            full_m.wait_recv()

        @pl.when(h < 3)
        def _():
            full_p.start()
            full_m.start()

        @pl.when(h == 3)
        def _():
            half_p, half_m = halves(buf, send, recv)
            half_p.start()
            half_m.start()

    def halves(buf, send, recv):
        far_p, far_m = lax.rem(z + NZ - 3, NZ), lax.rem(z + 3, NZ)
        half = CT // 2
        at_p, at_m = rows(far_p * CT, half), rows(far_m * CT + half, half)
        return (
            remote(buf.at[at_p, :], buf.at[at_p, :], send.at[0, 3], recv.at[NZ], up),
            remote(buf.at[at_m, :], buf.at[at_m, :], send.at[1, 3], recv.at[NZ + 1], down),
        )

    def ring_close(buf, send, recv):
        for copy in halves(buf, send, recv):
            copy.wait_recv()

    def ring_sent(buf, send, recv):
        for h in range(3):
            for way in range(2):
                at = rows(z * CT, CT)
                remote(buf.at[at, :], buf.at[at, :], send.at[way, h], recv.at[0], up).wait_send()
        for copy in halves(buf, send, recv):
            copy.wait_send()

    def exchanged(k, buf, at):
        for p in peers:
            here = buf.at[at(p), :]
            remote(here, here, x_send.at[k, 0], x_recv.at[k, p], other_c).wait_recv()

    def project_at(zz, ys):
        for yy in ys:
            w_arrived(zz, yy, 1 - c)
            project(zz, yy)

    for way in range(2):
        forward_w(1, own_y, way)
    w_arrived(z, far_y, c)
    for to in (up, down, other_c):
        go(w_copy(block(z, far_y, c), slot, to))
        slot += 1
    high = (ch_ref[pl.ds(z, 1), :], sh_ref[pl.ds(z, 1), :])
    sign = jnp.where(lax.broadcasted_iota(jnp.int32, (1, HD), 1) < HD // 2, -1.0, 1.0)
    ct_ref[...] = cl_ref[...] * high[0] - sl_ref[...] * high[1]
    st_ref[...] = (sl_ref[...] * high[0] + cl_ref[...] * high[1]) * sign
    project_at(z, (own_y, far_y))
    for h in range(1, 4):
        for way in range(2):
            if h < 3 or way == 0:
                forward_w(h + 1, own_y, way)
        for way in range(2):
            forward_w(h, far_y, way)
        if h == 3:
            exchanged(0, v_all, lambda p: rows(z * CT + p * TD, TD))
            ring(v_all, vr_send, vr_recv, jnp.int32(0))
        for sign in (-1, 1):
            project_at(z + sign * h, (own_y, far_y))
    forward_w(4, far_y, 1)
    project_at(z - 4, (own_y,))
    project_at(z + 4, (far_y,))
    ring(v_all, vr_send, vr_recv, jnp.int32(1))

    for p in range(NG):
        x = acc_k[:, p * HD : (p + 1) * HD] * r_all[mine, :]
        x = x * ct_ref[mine, :] + pltpu.roll(x, HD // 2, 1) * st_ref[mine, :]
        k_loc[p] = (x * key_fold).astype(BF16)
    at_me = rows(z * CT + g * TD, TD)
    for i, p in enumerate(peers):
        go(remote(k_loc.at[p], k_all.at[at_me, :], ka_send.at[i], ka_recv.at[g], z * NG + p))
    spread(2, do_ref, do_all)
    for i, p in enumerate(peers):
        go(r_copy(g, i, z * NG + p))
    go(t_copy(g, 0, other_c, tok_ref))
    go(t_copy(g, 1, other_y, tok_ref))
    k_all[at_me, :] = k_loc[g]
    ring(v_all, vr_send, vr_recv, jnp.int32(2))
    exchanged(1, q_all, lambda p: rows(p * TD, TD))
    for p in peers:
        here = k_all.at[rows(z * CT + p * TD, TD), :]
        remote(here, here, ka_send.at[0], ka_recv.at[p], other_c).wait_recv()

    ring(v_all, vr_send, vr_recv, jnp.int32(3))

    spans = [slice(t * QT, (t + 1) * QT) for t in range(CT // QT)]

    def each_head(body):
        def step(h, carry):
            body(h, rows(h * HD, HD))
            return carry

        lax.fori_loop(0, NG, step, 0)

    def scores(k, heads, span, masked):
        s = lax.dot_general(k, q_all[span, heads], NT, preferred_element_type=F32)
        if masked:
            key_at = lax.broadcasted_iota(jnp.int32, s.shape, 0)
            query_at = lax.broadcasted_iota(jnp.int32, s.shape, 1) + span.start
            s = jnp.where(key_at <= query_at, s, -1e30)
        return s

    def forward(j, first):
        v_t = v_all[rows(j * CT, CT), :].astype(F32).T.astype(BF16)
        vt_all[...] = v_t

        def body(h, heads):
            k = k_all[rows(j * CT, CT), :]
            all_s = [scores(k, heads, span, first) for span in spans]
            tops = [jnp.max(s, axis=0, keepdims=True) for s in all_s]
            if not first:
                before = [mx[h, :, span] for span in spans]
                tops = [jnp.maximum(a, b) for a, b in zip(before, tops)]
            es = [jnp.exp2(s - top) for s, top in zip(all_s, tops)]
            totals = [jnp.sum(e, axis=0, keepdims=True) for e in es]
            outs = [jnp.dot(vt_all[...], e.astype(BF16), preferred_element_type=F32) for e in es]
            for i, span in enumerate(spans):
                total, out = totals[i], outs[i]
                if not first:
                    fade = jnp.exp2(before[i] - tops[i])
                    total = total + den[h, :, span] * fade
                    out = out + ot[h, :, span] * fade
                mx[h, :, span] = tops[i]
                den[h, :, span] = total
                ot[h, :, span] = out

        each_head(body)

    def forward_step(d, carry):
        @pl.when(d < 4)
        def _():
            ring(k_all, kr_send, kr_recv, d)

        @pl.when(d == 4)
        def _():
            ring_close(v_all, vr_send, vr_recv)
            ring_close(k_all, kr_send, kr_recv)

        @pl.when(d == 0)
        def _():
            forward(z, True)

        @pl.when(jnp.logical_and(d > 0, d <= z))
        def _():
            forward(z - d, False)

        return carry

    lax.fori_loop(0, NZ, forward_step, 0)

    exchanged(2, do_all, lambda p: rows(p * TD, TD))
    for h in range(NG):
        for t in range(CT // QT):
            cols = slice(t * QT, (t + 1) * QT)
            heads = slice(h * HD, (h + 1) * HD)
            total = den[h, :, cols]
            out = ot[h, :, cols] / total
            d_out = do_all[cols, heads].astype(F32).T
            dlt[h, :, cols] = jnp.sum(out * d_out, axis=0, keepdims=True)
            mx[h, :, cols] = mx[h, :, cols] + jnp.log2(total)
            att_loc[cols, heads] = out.T.astype(BF16)
    for i, p in enumerate(peers):
        go(
            remote(
                att_loc.at[rows(p * TD, TD), :],
                att_ref.at[:, rows(g * NG * HD, NG * HD)],
                at_send.at[i], at_recv.at[g], z * NG + p,
            )
        )
    att_ref[:, rows(g * NG * HD, NG * HD)] = att_loc[mine, :]

    def backward(j, masked):
        dk_acc[...] = jnp.zeros_like(dk_acc)

        def body(h, heads):
            k, v = k_all[rows(j * CT, CT), :], v_all[rows(j * CT, CT), :]
            ps = [jnp.exp2(scores(k, heads, span, masked) - mx[h, :, span]) for span in spans]
            dps = [
                lax.dot_general(v, do_all[span, heads], NT, preferred_element_type=F32)
                for span in spans
            ]
            ds = [
                (p * (dp - dlt[h, :, span])).astype(BF16) for p, dp, span in zip(ps, dps, spans)
            ]
            dk_acc[...] += jnp.dot(
                jnp.concatenate(ds, axis=1), q_all[:, heads], preferred_element_type=F32
            )

        each_head(body)

    def dk_copy(j):
        return remote(dk_send.at[j], dk_recv.at[z], dk_ssem.at[j], dk_rsem.at[z], j * NG + g)

    def backward_step(j, carry):
        backward(j, False)
        dk_send[j] = (dk_acc[...] * score_scale).astype(BF16)
        dk_copy(j).start()
        return carry

    lax.fori_loop(0, z, backward_step, 0)

    t_y = (1 - y) * 2 + c
    t_copy(t_y, 1, other_y).wait_recv()
    go(t_copy(t_y, 2, other_c))

    backward(z, True)
    dk_acc[...] = dk_acc[...] * score_scale

    def dk_add(i, carry):
        remote(dk_send.at[0], dk_recv.at[i], dk_ssem.at[0], dk_rsem.at[i], up).wait_recv()
        dk_acc[...] += dk_recv[i].astype(F32)
        return carry

    for p in (y * 2 + (1 - c), (1 - y) * 2 + (1 - c)):
        t_copy(p, 0, other_c).wait_recv()
    for p in peers:
        r_copy(p, 0, other_c).wait_recv()
    lax.fori_loop(z + 1, NZ, dk_add, 0)
    for p in range(NG):
        part = slice(p * TD, (p + 1) * TD)
        dk = dk_acc[part, :]
        raw = dk * ct_ref[part, :] - pltpu.roll(dk, HD // 2, 1) * st_ref[part, :]
        rg_t[:, part] = (raw * r_all[part, :]).T.astype(BF16)

    half_k, half_f = HD // 2, CT // 2
    ways = ((0, up), (1, down))

    def term(zz):
        return jnp.dot(rg_t[...], tok_all[:, rows(zz * CT, CT)], preferred_element_type=F32)

    def mt_copy(s, way, k, to):
        src, dst = (mt_far, mt_got) if s == 0 else (mt_send.at[s - 1], mt_recv.at[s - 1])
        return remote(
            src.at[way, k], dst.at[way, k], mt_ssem.at[s, way, k], mt_rsem.at[s, way, k], to
        )

    far = term(lax.rem(z + 4, NZ))
    for k in range(2):
        for way, to in ways:
            part = slice(k * half_k, (k + 1) * half_k)
            mt_far[way, k] = far[part, way * half_f : (way + 1) * half_f].astype(BF16)
            go(mt_copy(0, way, k, to))
    for s in range(1, 4):
        for way, to in ways:
            mt_part[way] = term(lax.rem(z + (4 - s if way == 0 else 4 + s), NZ))
        for k in range(2):
            part = slice(k * half_k, (k + 1) * half_k)
            for way, to in ways:
                mt_copy(s - 1, way, k, to).wait_recv()
                if s == 1:
                    near = slice(way * half_f, (way + 1) * half_f)
                    mt_part[way, part, near] += mt_got[way, k].astype(F32)
                else:
                    mt_part[way, part, :] += mt_recv[s - 2, way, k].astype(F32)
                mt_send[s - 1, way, k] = mt_part[way, part, :].astype(BF16)
                go(mt_copy(s, way, k, to))
    mt_sum[...] = term(z)
    for k in range(2):
        part = slice(k * half_k, (k + 1) * half_k)
        for way, to in ways:
            mt_copy(3, way, k, to).wait_recv()
            mt_sum[part, :] += mt_recv[2, way, k].astype(F32)
    for i, p in enumerate(peers):
        go(
            remote(
                mt_sum.at[:, rows(p * TD, TD)], mt_x.at[g], mx_send.at[i], mx_recv.at[g], z * NG + p
            )
        )
    m_out_ref[:, rows(g * HD, HD)] = mt_sum[:, mine].T
    for p in peers:
        remote(mt_x.at[p], mt_x.at[p], mx_send.at[0], mx_recv.at[p], other_c).wait_recv()
        m_out_ref[:, rows(p * HD, HD)] = mt_x[p].T

    for p in peers:
        there = att_ref.at[:, rows(p * NG * HD, NG * HD)]
        remote(there, there, at_send.at[0], at_recv.at[p], other_c).wait_recv()
    for copy in sends:
        copy.wait_send()
    ring_sent(v_all, vr_send, vr_recv)
    ring_sent(k_all, kr_send, kr_recv)

    def dk_sent(j, carry):
        dk_copy(j).wait_send()
        return carry

    lax.fori_loop(0, z, dk_sent, 0)


def call(tokens, queries, values, out_grad, w_key, gain):
    width, key_width = tokens.shape[1], values.shape[1]
    dma = pltpu.SemaphoreType.DMA
    vmem = lambda shape, dtype: pltpu.VMEM(shape, dtype)
    tokens_all = NZ * CT
    return pl.pallas_call(
        kernel,
        out_shape=(
            jax.ShapeDtypeStruct(queries.shape, BF16),
            jax.ShapeDtypeStruct((TD, key_width), F32),
        ),
        in_specs=[pl.BlockSpec(memory_space=pltpu.VMEM)] * 10,
        out_specs=(pl.BlockSpec(memory_space=pltpu.VMEM),) * 2,
        scratch_shapes=[
            vmem((width, key_width), BF16),
            vmem((CT, width), BF16),
            vmem((CT, NG * HD), BF16),
            vmem((CT, NG * HD), BF16),
            vmem((tokens_all, HD), BF16),
            vmem((tokens_all, HD), BF16),
            vmem((NG, TD, HD), BF16),
            vmem((HD, CT), BF16),
            vmem((TD, key_width), F32),
            vmem((CT, HD), F32),
            vmem((CT, HD), F32),
            vmem((CT, HD), F32),
            vmem((NG, HD, CT), F32),
            vmem((NG, 1, CT), F32),
            vmem((NG, 1, CT), F32),
            vmem((NG, 1, CT), F32),
            vmem((CT, NG * HD), BF16),
            vmem((CT, HD), F32),
            vmem((NZ, CT, HD), BF16),
            vmem((NZ, CT, HD), BF16),
            vmem((HD, CT), BF16),
            vmem((2, 2, HD // 2, CT // 2), BF16),
            vmem((2, 2, HD // 2, CT // 2), BF16),
            vmem((3, 2, 2, HD // 2, CT), BF16),
            vmem((3, 2, 2, HD // 2, CT), BF16),
            vmem((2, HD, CT), F32),
            vmem((HD, CT), F32),
            vmem((NG, HD, TD), F32),
            dma((32,)), dma((32,)),
            dma((3, 3)), dma((3, NG)),
            dma((3,)), dma((NG,)),
            dma((3,)), dma((NG,)),
            dma((2, 4)), dma((NZ + 2,)),
            dma((2, 4)), dma((NZ + 2,)),
            dma((3,)), dma((NG,)),
            dma((NZ,)), dma((NZ,)),
            dma((4, 2, 2)), dma((4, 2, 2)),
            dma((3,)), dma((NG,)),
            dma((3,)), dma((NG,)),
        ],
        compiler_params=pltpu.CompilerParams(
            collective_id=0, has_side_effects=True, vmem_limit_bytes=56 << 20
        ),
    )(tokens, queries, values, out_grad, w_key, gain, *map(jnp.asarray, rope_parts()))


def shards(tokens, queries, values, out_grad, w_key, norm_gain, key_momentum, gain_momentum):
    w = w_key.astype(F32)
    gain = norm_gain.astype(F32)
    attended, m = call(tokens, queries, values, out_grad, w_key, gain[None, :])
    new_key_momentum = inertia * key_momentum + gain[:, None] * m
    new_key_weight = (w - step_size * new_key_momentum).astype(BF16)
    new_gain_momentum = inertia * gain_momentum + jnp.sum(w * m, axis=1)
    new_gain = (gain - step_size * new_gain_momentum).astype(BF16)
    return (attended, new_key_weight, new_key_momentum, new_gain, new_gain_momentum)


def solution(mesh):
    both, flat = P(BOTH, None), P(BOTH)
    return jax.shard_map(
        shards,
        mesh=mesh,
        in_specs=(both, both, both, both, both, flat, both, flat),
        out_specs=(both, both, both, flat, flat),
        check_vma=False,
    )
```

```python
import math

import jax
import jax.numpy as jnp
import numpy as np
from jax import lax
from jax.experimental import pallas as pl
from jax.experimental.pallas import tpu as pltpu
from jax.sharding import PartitionSpec as P

HD = 128
NZ = 8
NG = 4
TD = 128
CT = NG * TD
QT = 256
TP = 4
EARLY = (2, 3)
MP = 4
BOTH = ("replica", "shard")

epsilon = 1e-05
rope_base = 500000.0
inertia = 0.9
step_size = 0.01
score_scale = HD ** (-0.5)
key_fold = score_scale * math.log2(math.e)

F32 = jnp.float32
BF16 = jnp.bfloat16
MESH = pl.DeviceIdType.MESH
NT = (((1,), (1,)), ((), ()))


def rope_parts():
    half = HD // 2
    freq = np.exp(-math.log(rope_base) * np.arange(half) * (2.0 / HD))
    low = np.arange(CT)[:, None] * freq[None, :]
    high = (np.arange(NZ) * CT)[:, None] * freq[None, :]
    both = lambda a, b: np.concatenate([a, b], axis=1).astype(np.float32)
    return (
        both(np.cos(low), np.cos(low)),
        both(np.sin(low), np.sin(low)),
        both(np.cos(high), np.cos(high)),
        both(np.sin(high), np.sin(high)),
    )


def remote(src, dst, send, recv, device):
    return pltpu.make_async_remote_copy(
        src_ref=src,
        dst_ref=dst,
        send_sem=send,
        recv_sem=recv,
        device_id={"shard": device},
        device_id_type=MESH,
    )


def rows(start, size):
    return pl.ds(pl.multiple_of(start, size), size)


def kernel(
    tok_ref, q_ref, v_ref, do_ref, w_ref, gain_ref, cl_ref, sl_ref, ch_ref, sh_ref,
    att_ref, m_out_ref,
    w_all, tok_all, q_all, do_all, v_all, k_all, k_loc, vt_all,
    acc_k, ct_ref, st_ref, r_loc, r_all, ot, e_all, m_all, mx, den, dlt, att_loc, dk_acc, dk_send, dk_recv,
    rg_t, mt_far, mt_got, mt_send, mt_recv, mt_part, mt_sum, mt_x,
    w_send, w_recv, x_send, x_recv, t_send, t_recv, r_send, r_recv,
    vr_send, vr_recv, kr_send, kr_recv, ka_send, ka_recv,
    dk_ssem, dk_rsem, mt_ssem, mt_rsem, at_send, at_recv, mx_send, mx_recv,
):
    me = lax.axis_index("shard")
    z = me // NG
    g = lax.rem(me, NG)
    y = g // 2
    c = lax.rem(g, 2)
    zp = lax.rem(z + 1, NZ)
    zm = lax.rem(z + NZ - 1, NZ)
    up = zp * NG + g
    down = zm * NG + g
    other_y = z * NG + (1 - y) * 2 + c
    other_c = z * NG + y * 2 + (1 - c)
    peers = [lax.rem(g + i, NG) for i in range(1, NG)]

    own_w = rows(me * TD, TD)
    gain = jnp.broadcast_to(gain_ref[...], (TD, TD)).T
    for h in range(NG):
        cols = slice(h * HD, (h + 1) * HD)
        w_all[own_w, cols] = (w_ref[:, cols].astype(F32) * gain).astype(BF16)

    barrier = pltpu.get_barrier_semaphore()
    for i in range(1, NZ):
        pl.semaphore_signal(
            barrier, inc=1, device_id={"shard": lax.rem(z + i, NZ) * NG + g}, device_id_type=MESH
        )
    for p in peers:
        pl.semaphore_signal(barrier, inc=1, device_id={"shard": z * NG + p}, device_id_type=MESH)
    pl.semaphore_wait(barrier, NZ - 1 + NG - 1)

    def block(zz, yy, cc):
        return lax.rem(zz + 2 * NZ, NZ) * NG + yy * 2 + cc

    def w_copy(b, slot, device):
        here = w_all.at[rows(b * TD, TD), :]
        return remote(here, here, w_send.at[slot], w_recv.at[b], device)

    sends = []

    def go(copy):
        copy.start()
        sends.append(copy)

    for i, to in enumerate((up, down, other_y, other_c)):
        go(w_copy(me, i, to))

    mine = rows(g * TD, TD)
    for i, p in enumerate(peers):
        go(
            remote(
                v_ref.at[:, rows(p * HD, HD)],
                v_all.at[rows(z * CT + g * TD, TD), :],
                x_send.at[0, i], x_recv.at[0, g], z * NG + p,
            )
        )

    def spread(k, src, dst):
        for i, p in enumerate(peers):
            go(
                remote(
                    src.at[:, rows(p * NG * HD, NG * HD)],
                    dst.at[mine, :],
                    x_send.at[k, i], x_recv.at[k, g], z * NG + p,
                )
            )

    spread(1, q_ref, q_all)

    width = tok_ref.shape[1]
    piece = width // TP

    def t_copy(p, slot, i, device, src=None):
        cols = slice(i * piece, (i + 1) * piece)
        here = tok_all.at[rows(p * TD, TD), cols]
        src = here if src is None else src.at[:, cols]
        return remote(src, here, t_send.at[slot, i], t_recv.at[p, i], device)

    for i in range(TP):
        go(t_copy(g, 0, i, other_c, tok_ref))
    for i in range(EARLY[0]):
        go(t_copy(g, 1, i, other_y, tok_ref))

    v_all[rows(z * CT + g * TD, TD), :] = v_ref[:, rows(g * HD, HD)]
    q_all[mine, :] = q_ref[:, rows(g * NG * HD, NG * HD)]
    do_all[mine, :] = do_ref[:, rows(g * NG * HD, NG * HD)]
    tok_all[mine, :] = tok_ref[...]

    def add_squares(i, total):
        t = tok_ref[:, rows(i * 512, 512)].astype(F32)
        return total + jnp.sum(t * t, axis=1, keepdims=True)

    squares = lax.fori_loop(0, width // 512, add_squares, jnp.zeros((TD, 1), F32))
    r_mine = jnp.broadcast_to(lax.rsqrt(squares * (1.0 / width) + epsilon), (TD, HD))
    r_loc[...] = r_mine
    r_all[g] = r_mine.T[:8, :]

    def r_copy(p, i, device):
        here = r_all.at[p]
        return remote(here, here, r_send.at[i], r_recv.at[p], device)

    def project(zz, yy):
        cols = rows(block(zz, yy, 0) * TD, 2 * TD)
        acc_k[...] += jnp.dot(tok_ref[:, cols], w_all[cols, :], preferred_element_type=F32)

    def w_arrived(zz, yy, cc):
        w_copy(block(zz, yy, cc), 0, up).wait_recv()

    slot = 4

    def forward_w(h, yy, way):
        nonlocal slot
        zz = z + (-h if way == 0 else h)
        w_arrived(zz, yy, c)
        if h < 3 or (h == 3 and (way == 0) == (yy is own_y)):
            go(w_copy(block(zz, yy, c), slot, up if way == 0 else down))
            slot += 1
        go(w_copy(block(zz, yy, c), slot, other_c))
        slot += 1

    own_y, far_y = y, 1 - y
    acc_k[...] = jnp.zeros_like(acc_k)

    half = CT // 2
    ways = ((0, up), (1, down))

    def ring_copy(buf, send, recv, h, way, q):
        origin = lax.rem(z + NZ - h if way == 0 else z + h, NZ)
        here = buf.at[rows(origin * CT + q * half, half), :]
        to = up if way == 0 else down
        return remote(here, here, send.at[way, h, q], recv.at[origin, q], to)

    def ring(buf, send, recv, h):
        for q in range(2):
            for way in range(2):
                copy = ring_copy(buf, send, recv, h, way, q)
                pl.when(h > 0)(copy.wait_recv)
                pl.when(h < (4 if q == way else 3))(copy.start)

    def ring_close(buf, send, recv):
        for way in range(2):
            here = buf.at[rows(lax.rem(z + 4, NZ) * CT + way * half, half), :]
            sem = recv.at[lax.rem(z + 4, NZ), way]
            remote(here, here, send.at[way, 3, way], sem, up).wait_recv()

    def ring_sent(buf, send, recv):
        for h in range(4):
            for way in range(2):
                for q in range(2):
                    if h < 3 or q == way:
                        ring_copy(buf, send, recv, h, way, q).wait_send()

    def exchanged(k, buf, at):
        for p in peers:
            here = buf.at[at(p), :]
            remote(here, here, x_send.at[k, 0], x_recv.at[k, p], other_c).wait_recv()

    def project_at(zz, ys):
        for yy in ys:
            w_arrived(zz, yy, 1 - c)
            project(zz, yy)

    for way in range(2):
        forward_w(1, own_y, way)
    w_arrived(z, far_y, c)
    for to in (up, down, other_c):
        go(w_copy(block(z, far_y, c), slot, to))
        slot += 1
    high = (ch_ref[pl.ds(z, 1), :], sh_ref[pl.ds(z, 1), :])
    sign = jnp.where(lax.broadcasted_iota(jnp.int32, (1, HD), 1) < HD // 2, -1.0, 1.0)
    ct_ref[...] = cl_ref[...] * high[0] - sl_ref[...] * high[1]
    st_ref[...] = (sl_ref[...] * high[0] + cl_ref[...] * high[1]) * sign
    project_at(z, (own_y, far_y))
    for h in range(1, 4):
        for way in range(2):
            if h < 3 or way == 0:
                forward_w(h + 1, own_y, way)
        for way in range(2):
            forward_w(h, far_y, way)
        if h == 2:
            for i in range(*EARLY):
                go(t_copy(g, 1, i, other_y, tok_ref))
        if h == 3:
            exchanged(0, v_all, lambda p: rows(z * CT + p * TD, TD))
            ring(v_all, vr_send, vr_recv, jnp.int32(0))
        for sign in (-1, 1):
            project_at(z + sign * h, (own_y, far_y))
    forward_w(4, far_y, 1)
    project_at(z - 4, (own_y,))
    project_at(z + 4, (far_y,))
    ring(v_all, vr_send, vr_recv, jnp.int32(1))

    for p in range(NG):
        x = acc_k[:, p * HD : (p + 1) * HD] * r_loc[...]
        x = x * ct_ref[mine, :] + pltpu.roll(x, HD // 2, 1) * st_ref[mine, :]
        k_loc[p] = (x * key_fold).astype(BF16)
    at_me = rows(z * CT + g * TD, TD)
    for i, p in enumerate(peers):
        go(remote(k_loc.at[p], k_all.at[at_me, :], ka_send.at[i], ka_recv.at[g], z * NG + p))
    spread(2, do_ref, do_all)
    for i, p in enumerate(peers):
        go(r_copy(g, i, z * NG + p))
    for i in range(EARLY[1], TP):
        go(t_copy(g, 1, i, other_y, tok_ref))
    k_all[at_me, :] = k_loc[g]
    ring(v_all, vr_send, vr_recv, jnp.int32(2))
    exchanged(1, q_all, lambda p: rows(p * TD, TD))
    for p in peers:
        here = k_all.at[rows(z * CT + p * TD, TD), :]
        remote(here, here, ka_send.at[0], ka_recv.at[p], other_c).wait_recv()


    spans = [slice(t * QT, (t + 1) * QT) for t in range(CT // QT)]

    def each_head(body):
        def step(h, carry):
            body(h, rows(h * HD, HD))
            return carry

        lax.fori_loop(0, NG, step, 0)

    def scores(k, heads, span, masked):
        s = lax.dot_general(k, q_all[span, heads], NT, preferred_element_type=F32)
        if masked:
            key_at = lax.broadcasted_iota(jnp.int32, s.shape, 0)
            query_at = lax.broadcasted_iota(jnp.int32, s.shape, 1) + span.start
            s = jnp.where(key_at <= query_at, s, -1e30)
        return s

    def forward(j, first):
        v_t = v_all[rows(j * CT, CT), :].astype(F32).T.astype(BF16)
        vt_all[...] = v_t

        def body(h, heads):
            k = k_all[rows(j * CT, CT), :]
            all_s = [scores(k, heads, span, first) for span in spans]
            tops = [jnp.max(s, axis=0, keepdims=True) for s in all_s]
            if not first:
                before = [mx[h, :, span] for span in spans]
                tops = [jnp.maximum(a, b) for a, b in zip(before, tops)]
            es = [jnp.exp2(s - top) for s, top in zip(all_s, tops)]
            totals = [jnp.sum(e, axis=0, keepdims=True) for e in es]
            es = [e.astype(BF16) for e in es]
            outs = [jnp.dot(vt_all[...], e, preferred_element_type=F32) for e in es]
            for i, span in enumerate(spans):
                total, out = totals[i], outs[i]
                if not first:
                    fade = jnp.exp2(before[i] - tops[i])
                    total = total + den[h, :, span] * fade
                    out = out + ot[h, :, span] * fade
                e_all[j, h, :, span] = es[i]
                m_all[j, h, :, span] = tops[i]
                mx[h, :, span] = tops[i]
                den[h, :, span] = total
                ot[h, :, span] = out

        each_head(body)

    def forward_step(d, carry):
        @pl.when(d < 4)
        def _():
            ring(k_all, kr_send, kr_recv, d)

        @pl.when(d == 4)
        def _():
            ring_close(v_all, vr_send, vr_recv)
            ring_close(k_all, kr_send, kr_recv)

        @pl.when(d == 0)
        def _():
            forward(z, True)
            ring(v_all, vr_send, vr_recv, jnp.int32(3))

        def one(i, carry):
            forward(jnp.where(i == 0, z - d, z - NZ + d), False)
            return carry

        near = jnp.logical_and(d > 0, d <= z)
        far = jnp.logical_and(jnp.logical_and(d > 0, d < 4), z >= NZ - d)
        lax.fori_loop(0, near.astype(jnp.int32) + far.astype(jnp.int32), one, 0)
        return carry

    lax.fori_loop(0, NZ // 2 + 1, forward_step, 0)

    exchanged(2, do_all, lambda p: rows(p * TD, TD))
    for h in range(NG):
        for t in range(CT // QT):
            cols = slice(t * QT, (t + 1) * QT)
            heads = slice(h * HD, (h + 1) * HD)
            total = den[h, :, cols]
            out = ot[h, :, cols] / total
            d_out = do_all[cols, heads].astype(F32).T
            dlt[h, :, cols] = jnp.sum(out * d_out, axis=0, keepdims=True)
            mx[h, :, cols] = mx[h, :, cols] + jnp.log2(total)
            att_loc[cols, heads] = out.T.astype(BF16)
    for i, p in enumerate(peers):
        go(
            remote(
                att_loc.at[rows(p * TD, TD), :],
                att_ref.at[:, rows(g * NG * HD, NG * HD)],
                at_send.at[i], at_recv.at[g], z * NG + p,
            )
        )
    att_ref[:, rows(g * NG * HD, NG * HD)] = att_loc[mine, :]

    def backward(j):
        dk_acc[...] = jnp.zeros_like(dk_acc)

        def body(h, heads):
            v = v_all[rows(j * CT, CT), :]
            ps = [
                e_all[j, h, :, span].astype(F32) * jnp.exp2(m_all[j, h, :, span] - mx[h, :, span])
                for span in spans
            ]
            dps = [
                lax.dot_general(v, do_all[span, heads], NT, preferred_element_type=F32)
                for span in spans
            ]
            ds = [
                (p * (dp - dlt[h, :, span])).astype(BF16) for p, dp, span in zip(ps, dps, spans)
            ]
            dk_acc[...] += jnp.dot(
                jnp.concatenate(ds, axis=1), q_all[:, heads], preferred_element_type=F32
            )

        each_head(body)

    def dk_copy(j):
        return remote(dk_send.at[j], dk_recv.at[z], dk_ssem.at[j], dk_rsem.at[z], j * NG + g)

    def backward_step(j, carry):
        backward(j)
        dk_send[j] = (dk_acc[...] * score_scale).astype(BF16)
        dk_copy(j).start()
        return carry

    lax.fori_loop(0, z, backward_step, 0)

    t_y = (1 - y) * 2 + c
    for i in range(TP):
        t_copy(t_y, 1, i, other_y).wait_recv()
        go(t_copy(t_y, 2, i, other_c))

    backward(z)
    dk_acc[...] = dk_acc[...] * score_scale

    def dk_add(i, carry):
        remote(dk_send.at[0], dk_recv.at[i], dk_ssem.at[0], dk_rsem.at[i], up).wait_recv()
        dk_acc[...] += dk_recv[i].astype(F32)
        return carry

    for p in (y * 2 + (1 - c), (1 - y) * 2 + (1 - c)):
        for i in range(TP):
            t_copy(p, 0, i, other_c).wait_recv()
    for p in peers:
        r_copy(p, 0, other_c).wait_recv()
    lax.fori_loop(z + 1, NZ, dk_add, 0)
    for p in range(NG):
        part = slice(p * TD, (p + 1) * TD)
        dk = dk_acc[part, :]
        raw = dk * ct_ref[part, :] - pltpu.roll(dk, HD // 2, 1) * st_ref[part, :]
        rg_t[:, part] = (raw.T * r_all[p, :1, :]).astype(BF16)

    part_k, half_f = HD // MP, CT // 2

    def term(zz):
        return jnp.dot(rg_t[...], tok_all[:, rows(zz * CT, CT)], preferred_element_type=F32)

    def mt_copy(s, way, k, to):
        src, dst = (mt_far, mt_got) if s == 0 else (mt_send.at[s - 1], mt_recv.at[s - 1])
        return remote(
            src.at[way, k], dst.at[way, k], mt_ssem.at[s, way, k], mt_rsem.at[s, way, k], to
        )

    far = term(lax.rem(z + 4, NZ))
    for k in range(MP):
        for way, to in ways:
            part = slice(k * part_k, (k + 1) * part_k)
            mt_far[way, k] = far[part, way * half_f : (way + 1) * half_f].astype(BF16)
            go(mt_copy(0, way, k, to))
    for s in range(1, 4):
        for way, to in ways:
            mt_part[way] = term(lax.rem(z + (4 - s if way == 0 else 4 + s), NZ))
        for k in range(MP):
            part = slice(k * part_k, (k + 1) * part_k)
            for way, to in ways:
                mt_copy(s - 1, way, k, to).wait_recv()
                if s == 1:
                    near = slice(way * half_f, (way + 1) * half_f)
                    mt_part[way, part, near] += mt_got[way, k].astype(F32)
                else:
                    mt_part[way, part, :] += mt_recv[s - 2, way, k].astype(F32)
                mt_send[s - 1, way, k] = mt_part[way, part, :].astype(BF16)
                go(mt_copy(s, way, k, to))
    mt_sum[...] = term(z)
    for k in range(MP):
        part = slice(k * part_k, (k + 1) * part_k)
        for way, to in ways:
            mt_copy(3, way, k, to).wait_recv()
            mt_sum[part, :] += mt_recv[2, way, k].astype(F32)
        for i, p in enumerate(peers):
            here = mt_sum.at[part, rows(p * TD, TD)]
            go(remote(here, mt_x.at[g, part, :], mx_send.at[i, k], mx_recv.at[g, k], z * NG + p))
    m_out_ref[:, rows(g * HD, HD)] = mt_sum[:, mine].T
    for p in peers:
        for k in range(MP):
            here = mt_x.at[p, slice(k * part_k, (k + 1) * part_k), :]
            remote(here, here, mx_send.at[0, k], mx_recv.at[p, k], other_c).wait_recv()
        m_out_ref[:, rows(p * HD, HD)] = mt_x[p].T

    for p in peers:
        there = att_ref.at[:, rows(p * NG * HD, NG * HD)]
        remote(there, there, at_send.at[0], at_recv.at[p], other_c).wait_recv()
    for copy in sends:
        copy.wait_send()
    ring_sent(v_all, vr_send, vr_recv)
    ring_sent(k_all, kr_send, kr_recv)

    def dk_sent(j, carry):
        dk_copy(j).wait_send()
        return carry

    lax.fori_loop(0, z, dk_sent, 0)


def call(tokens, queries, values, out_grad, w_key, gain):
    width, key_width = tokens.shape[1], values.shape[1]
    dma = pltpu.SemaphoreType.DMA
    vmem = lambda shape, dtype: pltpu.VMEM(shape, dtype)
    tokens_all = NZ * CT
    return pl.pallas_call(
        kernel,
        out_shape=(
            jax.ShapeDtypeStruct(queries.shape, BF16),
            jax.ShapeDtypeStruct((TD, key_width), F32),
        ),
        in_specs=[pl.BlockSpec(memory_space=pltpu.VMEM)] * 10,
        out_specs=(pl.BlockSpec(memory_space=pltpu.VMEM),) * 2,
        scratch_shapes=[
            vmem((width, key_width), BF16),
            vmem((CT, width), BF16),
            vmem((CT, NG * HD), BF16),
            vmem((CT, NG * HD), BF16),
            vmem((tokens_all, HD), BF16),
            vmem((tokens_all, HD), BF16),
            vmem((NG, TD, HD), BF16),
            vmem((HD, CT), BF16),
            vmem((TD, key_width), F32),
            vmem((CT, HD), F32),
            vmem((CT, HD), F32),
            vmem((TD, HD), F32),
            vmem((NG, 8, TD), F32),
            vmem((NG, HD, CT), F32),
            vmem((NZ, NG, CT, CT), BF16),
            vmem((NZ, NG, 1, CT), F32),
            vmem((NG, 1, CT), F32),
            vmem((NG, 1, CT), F32),
            vmem((NG, 1, CT), F32),
            vmem((CT, NG * HD), BF16),
            vmem((CT, HD), F32),
            vmem((NZ, CT, HD), BF16),
            vmem((NZ, CT, HD), BF16),
            vmem((HD, CT), BF16),
            vmem((2, MP, HD // MP, CT // 2), BF16),
            vmem((2, MP, HD // MP, CT // 2), BF16),
            vmem((3, 2, MP, HD // MP, CT), BF16),
            vmem((3, 2, MP, HD // MP, CT), BF16),
            vmem((2, HD, CT), F32),
            vmem((HD, CT), F32),
            vmem((NG, HD, TD), F32),
            dma((32,)), dma((32,)),
            dma((3, 3)), dma((3, NG)),
            dma((3, TP)), dma((NG, TP)),
            dma((3,)), dma((NG,)),
            dma((2, 4, 2)), dma((NZ, 2)),
            dma((2, 4, 2)), dma((NZ, 2)),
            dma((3,)), dma((NG,)),
            dma((NZ,)), dma((NZ,)),
            dma((4, 2, MP)), dma((4, 2, MP)),
            dma((3,)), dma((NG,)),
            dma((3, MP)), dma((NG, MP)),
        ],
        compiler_params=pltpu.CompilerParams(
            collective_id=0, has_side_effects=True, vmem_limit_bytes=56 << 20
        ),
    )(tokens, queries, values, out_grad, w_key, gain, *map(jnp.asarray, rope_parts()))


def shards(tokens, queries, values, out_grad, w_key, norm_gain, key_momentum, gain_momentum):
    w = w_key.astype(F32)
    gain = norm_gain.astype(F32)
    attended, m = call(tokens, queries, values, out_grad, w_key, gain[None, :])
    new_key_momentum = inertia * key_momentum + gain[:, None] * m
    new_key_weight = (w - step_size * new_key_momentum).astype(BF16)
    new_gain_momentum = inertia * gain_momentum + jnp.sum(w * m, axis=1)
    new_gain = (gain - step_size * new_gain_momentum).astype(BF16)
    return (attended, new_key_weight, new_key_momentum, new_gain, new_gain_momentum)


def solution(mesh):
    both, flat = P(BOTH, None), P(BOTH)
    return jax.shard_map(
        shards,
        mesh=mesh,
        in_specs=(both, both, both, both, both, flat, both, flat),
        out_specs=(both, both, both, flat, flat),
        check_vma=False,
    )
```

```python
import math

import jax
import jax.numpy as jnp
import numpy as np
from jax import lax
from jax.experimental import pallas as pl
from jax.experimental.pallas import tpu as pltpu
from jax.sharding import PartitionSpec as P

HD = 128
NZ = 8
NG = 4
TD = 128
CT = NG * TD
QT = 256
TP = 4
EARLY = (2, 3)
MP = 4
BOTH = ("replica", "shard")

epsilon = 1e-05
rope_base = 500000.0
inertia = 0.9
step_size = 0.01
score_scale = HD ** (-0.5)
key_fold = score_scale * math.log2(math.e)

F32 = jnp.float32
BF16 = jnp.bfloat16
MESH = pl.DeviceIdType.MESH
NT = (((1,), (1,)), ((), ()))


def rope_parts():
    half = HD // 2
    freq = np.exp(-math.log(rope_base) * np.arange(half) * (2.0 / HD))
    low = np.arange(CT)[:, None] * freq[None, :]
    high = (np.arange(NZ) * CT)[:, None] * freq[None, :]
    both = lambda a, b: np.concatenate([a, b], axis=1).astype(np.float32)
    return (
        both(np.cos(low), np.cos(low)),
        both(np.sin(low), np.sin(low)),
        both(np.cos(high), np.cos(high)),
        both(np.sin(high), np.sin(high)),
    )


def remote(src, dst, send, recv, device):
    return pltpu.make_async_remote_copy(
        src_ref=src,
        dst_ref=dst,
        send_sem=send,
        recv_sem=recv,
        device_id={"shard": device},
        device_id_type=MESH,
    )


def rows(start, size):
    return pl.ds(pl.multiple_of(start, size), size)


def kernel(
    tok_ref, q_ref, v_ref, do_ref, w_ref, gain_ref, cl_ref, sl_ref, ch_ref, sh_ref,
    att_ref, m_out_ref,
    w_all, tok_all, q_all, do_all, v_all, k_all, k_loc, vt_all,
    acc_k, ct_ref, st_ref, r_loc, r_all, ot, e_all, m_all, mx, den, dlt, att_loc, dk_acc, dk_send, dk_recv,
    rg_t, mt_far, mt_got, mt_send, mt_recv, mt_part, mt_sum, mt_x,
    w_send, w_recv, x_send, x_recv, t_send, t_recv, r_send, r_recv,
    vr_send, vr_recv, kr_send, kr_recv, ka_send, ka_recv,
    dk_ssem, dk_rsem, mt_ssem, mt_rsem, at_send, at_recv, mx_send, mx_recv,
):
    me = lax.axis_index("shard")
    z = me // NG
    g = lax.rem(me, NG)
    y = g // 2
    c = lax.rem(g, 2)
    zp = lax.rem(z + 1, NZ)
    zm = lax.rem(z + NZ - 1, NZ)
    up = zp * NG + g
    down = zm * NG + g
    other_y = z * NG + (1 - y) * 2 + c
    other_c = z * NG + y * 2 + (1 - c)
    peers = [lax.rem(g + i, NG) for i in range(1, NG)]

    own_w = rows(me * TD, TD)
    gain = jnp.broadcast_to(gain_ref[...], (TD, TD)).T
    for h in range(NG):
        cols = slice(h * HD, (h + 1) * HD)
        w_all[own_w, cols] = (w_ref[:, cols].astype(F32) * gain).astype(BF16)

    barrier = pltpu.get_barrier_semaphore()
    for i in range(1, NZ):
        pl.semaphore_signal(
            barrier, inc=1, device_id={"shard": lax.rem(z + i, NZ) * NG + g}, device_id_type=MESH
        )
    for p in peers:
        pl.semaphore_signal(barrier, inc=1, device_id={"shard": z * NG + p}, device_id_type=MESH)
    pl.semaphore_wait(barrier, NZ - 1 + NG - 1)

    def block(zz, yy, cc):
        return lax.rem(zz + 2 * NZ, NZ) * NG + yy * 2 + cc

    def w_copy(b, slot, device):
        here = w_all.at[rows(b * TD, TD), :]
        return remote(here, here, w_send.at[slot], w_recv.at[b], device)

    sends = []

    def go(copy):
        copy.start()
        sends.append(copy)

    for i, to in enumerate((up, down, other_y, other_c)):
        go(w_copy(me, i, to))

    mine = rows(g * TD, TD)
    for i, p in enumerate(peers):
        go(
            remote(
                v_ref.at[:, rows(p * HD, HD)],
                v_all.at[rows(z * CT + g * TD, TD), :],
                x_send.at[0, i], x_recv.at[0, g], z * NG + p,
            )
        )

    def spread(k, src, dst):
        for i, p in enumerate(peers):
            go(
                remote(
                    src.at[:, rows(p * NG * HD, NG * HD)],
                    dst.at[mine, :],
                    x_send.at[k, i], x_recv.at[k, g], z * NG + p,
                )
            )

    spread(1, q_ref, q_all)

    width = tok_ref.shape[1]
    piece = width // TP

    def t_copy(p, slot, i, device, src=None):
        cols = slice(i * piece, (i + 1) * piece)
        here = tok_all.at[rows(p * TD, TD), cols]
        src = here if src is None else src.at[:, cols]
        return remote(src, here, t_send.at[slot, i], t_recv.at[p, i], device)

    for i in range(TP):
        go(t_copy(g, 0, i, other_c, tok_ref))
    for i in range(EARLY[0]):
        go(t_copy(g, 1, i, other_y, tok_ref))

    v_all[rows(z * CT + g * TD, TD), :] = v_ref[:, rows(g * HD, HD)]
    q_all[mine, :] = q_ref[:, rows(g * NG * HD, NG * HD)]
    do_all[mine, :] = do_ref[:, rows(g * NG * HD, NG * HD)]
    tok_all[mine, :] = tok_ref[...]

    def add_squares(i, total):
        t = tok_ref[:, rows(i * 512, 512)].astype(F32)
        return total + jnp.sum(t * t, axis=1, keepdims=True)

    squares = lax.fori_loop(0, width // 512, add_squares, jnp.zeros((TD, 1), F32))
    r_mine = jnp.broadcast_to(lax.rsqrt(squares * (1.0 / width) + epsilon), (TD, HD))
    r_loc[...] = r_mine
    r_all[g] = r_mine.T[:8, :]

    def r_copy(p, i, device):
        here = r_all.at[p]
        return remote(here, here, r_send.at[i], r_recv.at[p], device)

    def project(zz, yy):
        cols = rows(block(zz, yy, 0) * TD, 2 * TD)
        acc_k[...] += jnp.dot(tok_ref[:, cols], w_all[cols, :], preferred_element_type=F32)

    def w_arrived(zz, yy, cc):
        w_copy(block(zz, yy, cc), 0, up).wait_recv()

    slot = 4

    def forward_w(h, yy, way):
        nonlocal slot
        zz = z + (-h if way == 0 else h)
        w_arrived(zz, yy, c)
        if h < 3 or (h == 3 and (way == 0) == (yy is own_y)):
            go(w_copy(block(zz, yy, c), slot, up if way == 0 else down))
            slot += 1
        go(w_copy(block(zz, yy, c), slot, other_c))
        slot += 1

    own_y, far_y = y, 1 - y
    acc_k[...] = jnp.zeros_like(acc_k)

    half = CT // 2
    ways = ((0, up), (1, down))

    def ring_copy(buf, send, recv, h, way, q):
        origin = lax.rem(z + NZ - h if way == 0 else z + h, NZ)
        here = buf.at[rows(origin * CT + q * half, half), :]
        to = up if way == 0 else down
        return remote(here, here, send.at[way, h, q], recv.at[origin, q], to)

    def ring(buf, send, recv, h):
        for q in range(2):
            for way in range(2):
                copy = ring_copy(buf, send, recv, h, way, q)
                pl.when(h > 0)(copy.wait_recv)
                pl.when(h < (4 if q == way else 3))(copy.start)

    def ring_close(buf, send, recv):
        for way in range(2):
            here = buf.at[rows(lax.rem(z + 4, NZ) * CT + way * half, half), :]
            sem = recv.at[lax.rem(z + 4, NZ), way]
            remote(here, here, send.at[way, 3, way], sem, up).wait_recv()

    def ring_sent(buf, send, recv):
        for h in range(4):
            for way in range(2):
                for q in range(2):
                    if h < 3 or q == way:
                        ring_copy(buf, send, recv, h, way, q).wait_send()

    def exchanged(k, buf, at):
        for p in peers:
            here = buf.at[at(p), :]
            remote(here, here, x_send.at[k, 0], x_recv.at[k, p], other_c).wait_recv()

    def project_at(zz, ys):
        for yy in ys:
            w_arrived(zz, yy, 1 - c)
            project(zz, yy)

    w_arrived(z, far_y, c)
    for to in (up, down, other_c):
        go(w_copy(block(z, far_y, c), slot, to))
        slot += 1
    for way in range(2):
        forward_w(1, own_y, way)
    high = (ch_ref[pl.ds(z, 1), :], sh_ref[pl.ds(z, 1), :])
    sign = jnp.where(lax.broadcasted_iota(jnp.int32, (1, HD), 1) < HD // 2, -1.0, 1.0)
    ct_ref[...] = cl_ref[...] * high[0] - sl_ref[...] * high[1]
    st_ref[...] = (sl_ref[...] * high[0] + cl_ref[...] * high[1]) * sign
    project_at(z, (own_y, far_y))
    for h in range(1, 4):
        for way in range(2):
            if h < 3 or way == 0:
                forward_w(h + 1, own_y, way)
        for way in range(2):
            forward_w(h, far_y, way)
        if h == 2:
            for i in range(*EARLY):
                go(t_copy(g, 1, i, other_y, tok_ref))
        if h == 2:
            exchanged(0, v_all, lambda p: rows(z * CT + p * TD, TD))
        if h > 1:
            ring(v_all, vr_send, vr_recv, jnp.int32(h - 2))
        for sign in (-1, 1):
            project_at(z + sign * h, (own_y, far_y))
    forward_w(4, far_y, 1)
    project_at(z - 4, (own_y,))
    project_at(z + 4, (far_y,))
    ring(v_all, vr_send, vr_recv, jnp.int32(2))

    for p in range(NG):
        x = acc_k[:, p * HD : (p + 1) * HD] * r_loc[...]
        x = x * ct_ref[mine, :] + pltpu.roll(x, HD // 2, 1) * st_ref[mine, :]
        k_loc[p] = (x * key_fold).astype(BF16)
    at_me = rows(z * CT + g * TD, TD)
    for i, p in enumerate(peers):
        go(remote(k_loc.at[p], k_all.at[at_me, :], ka_send.at[i], ka_recv.at[g], z * NG + p))
    spread(2, do_ref, do_all)
    for i, p in enumerate(peers):
        go(r_copy(g, i, z * NG + p))
    for i in range(EARLY[1], TP):
        go(t_copy(g, 1, i, other_y, tok_ref))
    k_all[at_me, :] = k_loc[g]
    ring(v_all, vr_send, vr_recv, jnp.int32(3))
    exchanged(1, q_all, lambda p: rows(p * TD, TD))
    for p in peers:
        here = k_all.at[rows(z * CT + p * TD, TD), :]
        remote(here, here, ka_send.at[0], ka_recv.at[p], other_c).wait_recv()


    spans = [slice(t * QT, (t + 1) * QT) for t in range(CT // QT)]

    def each_head(body):
        def step(h, carry):
            body(h, rows(h * HD, HD))
            return carry

        lax.fori_loop(0, NG, step, 0)

    def scores(k, heads, span, masked):
        s = lax.dot_general(k, q_all[span, heads], NT, preferred_element_type=F32)
        if masked:
            key_at = lax.broadcasted_iota(jnp.int32, s.shape, 0)
            query_at = lax.broadcasted_iota(jnp.int32, s.shape, 1) + span.start
            s = jnp.where(key_at <= query_at, s, -1e30)
        return s

    def forward(j, first):
        v_t = v_all[rows(j * CT, CT), :].astype(F32).T.astype(BF16)
        vt_all[...] = v_t

        def body(h, heads):
            k = k_all[rows(j * CT, CT), :]
            all_s = [scores(k, heads, span, first) for span in spans]
            tops = [jnp.max(s, axis=0, keepdims=True) for s in all_s]
            if not first:
                before = [mx[h, :, span] for span in spans]
                tops = [jnp.maximum(a, b) for a, b in zip(before, tops)]
            es = [jnp.exp2(s - top) for s, top in zip(all_s, tops)]
            totals = [jnp.sum(e, axis=0, keepdims=True) for e in es]
            es = [e.astype(BF16) for e in es]
            outs = [jnp.dot(vt_all[...], e, preferred_element_type=F32) for e in es]
            for i, span in enumerate(spans):
                total, out = totals[i], outs[i]
                if not first:
                    fade = jnp.exp2(before[i] - tops[i])
                    total = total + den[h, :, span] * fade
                    out = out + ot[h, :, span] * fade
                e_all[j, h, :, span] = es[i]
                m_all[j, h, :, span] = tops[i]
                mx[h, :, span] = tops[i]
                den[h, :, span] = total
                ot[h, :, span] = out

        each_head(body)

    def forward_step(d, carry):
        @pl.when(d < 4)
        def _():
            ring(k_all, kr_send, kr_recv, d)

        @pl.when(d == 4)
        def _():
            ring_close(v_all, vr_send, vr_recv)
            ring_close(k_all, kr_send, kr_recv)

        @pl.when(d == 0)
        def _():
            forward(z, True)

        def one(i, carry):
            forward(jnp.where(i == 0, z - d, z - NZ + d), False)
            return carry

        near = jnp.logical_and(d > 0, d <= z)
        far = jnp.logical_and(jnp.logical_and(d > 0, d < 4), z >= NZ - d)
        lax.fori_loop(0, near.astype(jnp.int32) + far.astype(jnp.int32), one, 0)
        return carry

    lax.fori_loop(0, NZ // 2 + 1, forward_step, 0)

    exchanged(2, do_all, lambda p: rows(p * TD, TD))
    for h in range(NG):
        for t in range(CT // QT):
            cols = slice(t * QT, (t + 1) * QT)
            heads = slice(h * HD, (h + 1) * HD)
            total = den[h, :, cols]
            out = ot[h, :, cols] / total
            d_out = do_all[cols, heads].astype(F32).T
            dlt[h, :, cols] = jnp.sum(out * d_out, axis=0, keepdims=True)
            mx[h, :, cols] = mx[h, :, cols] + jnp.log2(total)
            att_loc[cols, heads] = out.T.astype(BF16)
    for i, p in enumerate(peers):
        go(
            remote(
                att_loc.at[rows(p * TD, TD), :],
                att_ref.at[:, rows(g * NG * HD, NG * HD)],
                at_send.at[i], at_recv.at[g], z * NG + p,
            )
        )
    att_ref[:, rows(g * NG * HD, NG * HD)] = att_loc[mine, :]

    def backward(j):
        dk_acc[...] = jnp.zeros_like(dk_acc)

        def body(h, heads):
            v = v_all[rows(j * CT, CT), :]
            ps = [
                e_all[j, h, :, span].astype(F32) * jnp.exp2(m_all[j, h, :, span] - mx[h, :, span])
                for span in spans
            ]
            dps = [
                lax.dot_general(v, do_all[span, heads], NT, preferred_element_type=F32)
                for span in spans
            ]
            ds = [
                (p * (dp - dlt[h, :, span])).astype(BF16) for p, dp, span in zip(ps, dps, spans)
            ]
            dk_acc[...] += jnp.dot(
                jnp.concatenate(ds, axis=1), q_all[:, heads], preferred_element_type=F32
            )

        each_head(body)

    def dk_copy(j):
        return remote(dk_send.at[j], dk_recv.at[z], dk_ssem.at[j], dk_rsem.at[z], j * NG + g)

    def backward_step(j, carry):
        backward(j)
        dk_send[j] = (dk_acc[...] * score_scale).astype(BF16)
        dk_copy(j).start()
        return carry

    lax.fori_loop(0, z, backward_step, 0)

    t_y = (1 - y) * 2 + c
    for i in range(TP):
        t_copy(t_y, 1, i, other_y).wait_recv()
        go(t_copy(t_y, 2, i, other_c))

    backward(z)
    dk_acc[...] = dk_acc[...] * score_scale

    def dk_add(i, carry):
        remote(dk_send.at[0], dk_recv.at[i], dk_ssem.at[0], dk_rsem.at[i], up).wait_recv()
        dk_acc[...] += dk_recv[i].astype(F32)
        return carry

    for p in (y * 2 + (1 - c), (1 - y) * 2 + (1 - c)):
        for i in range(TP):
            t_copy(p, 0, i, other_c).wait_recv()
    for p in peers:
        r_copy(p, 0, other_c).wait_recv()
    lax.fori_loop(z + 1, NZ, dk_add, 0)
    for p in range(NG):
        part = slice(p * TD, (p + 1) * TD)
        dk = dk_acc[part, :]
        raw = dk * ct_ref[part, :] - pltpu.roll(dk, HD // 2, 1) * st_ref[part, :]
        rg_t[:, part] = (raw.T * r_all[p, :1, :]).astype(BF16)

    part_k, half_f = HD // MP, CT // 2

    def term(zz):
        return jnp.dot(rg_t[...], tok_all[:, rows(zz * CT, CT)], preferred_element_type=F32)

    def mt_copy(s, way, k, to):
        src, dst = (mt_far, mt_got) if s == 0 else (mt_send.at[s - 1], mt_recv.at[s - 1])
        return remote(
            src.at[way, k], dst.at[way, k], mt_ssem.at[s, way, k], mt_rsem.at[s, way, k], to
        )

    far = term(lax.rem(z + 4, NZ))
    for k in range(MP):
        for way, to in ways:
            part = slice(k * part_k, (k + 1) * part_k)
            mt_far[way, k] = far[part, way * half_f : (way + 1) * half_f].astype(BF16)
            go(mt_copy(0, way, k, to))
    for s in range(1, 4):
        for way, to in ways:
            mt_part[way] = term(lax.rem(z + (4 - s if way == 0 else 4 + s), NZ))
        for k in range(MP):
            part = slice(k * part_k, (k + 1) * part_k)
            for way, to in ways:
                mt_copy(s - 1, way, k, to).wait_recv()
                if s == 1:
                    near = slice(way * half_f, (way + 1) * half_f)
                    mt_part[way, part, near] += mt_got[way, k].astype(F32)
                else:
                    mt_part[way, part, :] += mt_recv[s - 2, way, k].astype(F32)
                mt_send[s - 1, way, k] = mt_part[way, part, :].astype(BF16)
                go(mt_copy(s, way, k, to))
    mt_sum[...] = term(z)
    for k in range(MP):
        part = slice(k * part_k, (k + 1) * part_k)
        for way, to in ways:
            mt_copy(3, way, k, to).wait_recv()
            mt_sum[part, :] += mt_recv[2, way, k].astype(F32)
        for i, p in enumerate(peers):
            here = mt_sum.at[part, rows(p * TD, TD)]
            go(remote(here, mt_x.at[g, part, :], mx_send.at[i, k], mx_recv.at[g, k], z * NG + p))
    m_out_ref[:, rows(g * HD, HD)] = mt_sum[:, mine].T
    for p in peers:
        for k in range(MP):
            here = mt_x.at[p, slice(k * part_k, (k + 1) * part_k), :]
            remote(here, here, mx_send.at[0, k], mx_recv.at[p, k], other_c).wait_recv()
        m_out_ref[:, rows(p * HD, HD)] = mt_x[p].T

    for p in peers:
        there = att_ref.at[:, rows(p * NG * HD, NG * HD)]
        remote(there, there, at_send.at[0], at_recv.at[p], other_c).wait_recv()
    for copy in sends:
        copy.wait_send()
    ring_sent(v_all, vr_send, vr_recv)
    ring_sent(k_all, kr_send, kr_recv)

    def dk_sent(j, carry):
        dk_copy(j).wait_send()
        return carry

    lax.fori_loop(0, z, dk_sent, 0)


def call(tokens, queries, values, out_grad, w_key, gain):
    width, key_width = tokens.shape[1], values.shape[1]
    dma = pltpu.SemaphoreType.DMA
    vmem = lambda shape, dtype: pltpu.VMEM(shape, dtype)
    tokens_all = NZ * CT
    return pl.pallas_call(
        kernel,
        out_shape=(
            jax.ShapeDtypeStruct(queries.shape, BF16),
            jax.ShapeDtypeStruct((TD, key_width), F32),
        ),
        in_specs=[pl.BlockSpec(memory_space=pltpu.VMEM)] * 10,
        out_specs=(pl.BlockSpec(memory_space=pltpu.VMEM),) * 2,
        scratch_shapes=[
            vmem((width, key_width), BF16),
            vmem((CT, width), BF16),
            vmem((CT, NG * HD), BF16),
            vmem((CT, NG * HD), BF16),
            vmem((tokens_all, HD), BF16),
            vmem((tokens_all, HD), BF16),
            vmem((NG, TD, HD), BF16),
            vmem((HD, CT), BF16),
            vmem((TD, key_width), F32),
            vmem((CT, HD), F32),
            vmem((CT, HD), F32),
            vmem((TD, HD), F32),
            vmem((NG, 8, TD), F32),
            vmem((NG, HD, CT), F32),
            vmem((NZ, NG, CT, CT), BF16),
            vmem((NZ, NG, 1, CT), F32),
            vmem((NG, 1, CT), F32),
            vmem((NG, 1, CT), F32),
            vmem((NG, 1, CT), F32),
            vmem((CT, NG * HD), BF16),
            vmem((CT, HD), F32),
            vmem((NZ, CT, HD), BF16),
            vmem((NZ, CT, HD), BF16),
            vmem((HD, CT), BF16),
            vmem((2, MP, HD // MP, CT // 2), BF16),
            vmem((2, MP, HD // MP, CT // 2), BF16),
            vmem((3, 2, MP, HD // MP, CT), BF16),
            vmem((3, 2, MP, HD // MP, CT), BF16),
            vmem((2, HD, CT), F32),
            vmem((HD, CT), F32),
            vmem((NG, HD, TD), F32),
            dma((32,)), dma((32,)),
            dma((3, 3)), dma((3, NG)),
            dma((3, TP)), dma((NG, TP)),
            dma((3,)), dma((NG,)),
            dma((2, 4, 2)), dma((NZ, 2)),
            dma((2, 4, 2)), dma((NZ, 2)),
            dma((3,)), dma((NG,)),
            dma((NZ,)), dma((NZ,)),
            dma((4, 2, MP)), dma((4, 2, MP)),
            dma((3,)), dma((NG,)),
            dma((3, MP)), dma((NG, MP)),
        ],
        compiler_params=pltpu.CompilerParams(
            collective_id=0, has_side_effects=True, vmem_limit_bytes=56 << 20
        ),
    )(tokens, queries, values, out_grad, w_key, gain, *map(jnp.asarray, rope_parts()))


def shards(tokens, queries, values, out_grad, w_key, norm_gain, key_momentum, gain_momentum):
    w = w_key.astype(F32)
    gain = norm_gain.astype(F32)
    attended, m = call(tokens, queries, values, out_grad, w_key, gain[None, :])
    new_key_momentum = inertia * key_momentum + gain[:, None] * m
    new_key_weight = (w - step_size * new_key_momentum).astype(BF16)
    new_gain_momentum = inertia * gain_momentum + jnp.sum(w * m, axis=1)
    new_gain = (gain - step_size * new_gain_momentum).astype(BF16)
    return (attended, new_key_weight, new_key_momentum, new_gain, new_gain_momentum)


def solution(mesh):
    both, flat = P(BOTH, None), P(BOTH)
    return jax.shard_map(
        shards,
        mesh=mesh,
        in_specs=(both, both, both, both, both, flat, both, flat),
        out_specs=(both, both, both, flat, flat),
        check_vma=False,
    )
```
